256 devices in a mesh: slab: 128 (over y, z, x), energy: 2 (over core).
Axes of the slice: x: 4, y: 4, z: 8, core: 2. Of those that a mesh axis runs over, the one named last changes fastest.
Arguments:
- onsite_energy: float32 [256, 128], P('slab'), may hold values from -0.3 to 0.3
- onsite_mixing: float32 [256, 128, 128], P('slab'), may hold values from -0.15625 to 0.15625
- hop_strength: float32 [256, 128], P('slab'), may hold values from 0.8 to 1.2
- hop_mixing: float32 [256, 128, 128], P('slab'), may hold values from -0.15625 to 0.15625
- energy: float32 [2], P('energy'), parts along dimension 0, may hold values from -0.4 to 0.4
- broadening: float32 [2], P('energy'), parts along dimension 0, may hold values from 0.01 to 0.025
Outputs:
- green_real: float32 [512, 128, 128], P(('energy', 'slab')), parts along dimension 0
- green_imag: float32 [512, 128, 128], P(('energy', 'slab')), parts along dimension 0
The draws below stay inside these ranges and needn't reach their ends.
There are 2 independent parts, one for each index of `energy`. The reference program is written for one: setup_inputs(seed, part) draws one part's arguments, and reference() takes and returns one part's arrays. A program takes and returns all parts, laid end to end along the dimension named above; an argument that names none is the same for every part. Nothing has to cross between parts.
All inputs are finite; a program needn't handle non-finite values.
Results may differ from the reference program's by a relative error of at most 0.0007.
Values sent between devices are 32-bit elements; how exact they have to be, the bound alone decides.
A program may use at most 128 MiB of HBM per device.

```python
import math
import jax
import jax.numpy as jnp
from jax import lax

ORB = 128
SLABS = 256


def steps_of(own_key, extent, cuts, smallest, largest):
    loudness = 1.0
    for position, shards_of in cuts:
        heights = jax.random.uniform(jax.random.fold_in(jax.random.fold_in(own_key, 6), position), (shards_of,), jnp.float32, smallest / len(cuts), largest / len(cuts))
        loudness = loudness * jnp.repeat(jnp.exp(heights), extent[position] // shards_of).reshape((-1,) + (1,) * (len(extent) - 1 - position))
    return loudness


def centred(rng, shape, scale, bound, pieces=(), kind=jnp.bfloat16):
    drawn = jax.random.normal(rng, shape, jnp.float32) * scale
    if len(pieces) > 0:
        drawn = steps_of(rng, shape, pieces, -0.22, 0.18) * drawn
    return jnp.clip(drawn, min=-bound, max=bound).astype(kind)


def setup_inputs(seed: int = 0, part: int = 0) -> dict:
    seeds = jax.random.split(jax.random.key(seed), 7)
    own_keys = jax.random.split(jax.random.fold_in(seeds[6], part), 7)
    onsite_energy = jnp.clip(jax.random.uniform(seeds[0], (SLABS, ORB), jnp.float32, -0.3, 0.3) * steps_of(seeds[0], (SLABS, ORB), ((0, 128),), -0.4, 0.0), -0.3, 0.3)
    onsite_mixing = centred(seeds[1], (SLABS, ORB, ORB), (10 * ORB) ** -0.5, 0.15625, ((0, 128),), jnp.float32)
    hop_strength = jnp.clip(0.8 + 0.40000004 * jax.random.uniform(seeds[2], (SLABS, ORB), jnp.float32) ** steps_of(seeds[2], (SLABS, ORB), ((0, 128),), -0.2, 0.2), 0.8, 1.2)
    hop_mixing = centred(seeds[3], (SLABS, ORB, ORB), (10 * ORB) ** -0.5, 0.15625, ((0, 128),), jnp.float32)
    energy = jnp.clip(jax.random.uniform(own_keys[4], (1,), jnp.float32, -0.4, 0.4), -0.4, 0.4)
    broadening = jnp.clip(jnp.exp(jax.random.uniform(own_keys[5], (1,), jnp.float32, math.log(0.01), math.log(0.025))), 0.01, 0.025)
    return dict(onsite_energy=onsite_energy, onsite_mixing=onsite_mixing, hop_strength=hop_strength, hop_mixing=hop_mixing, energy=energy, broadening=broadening)


def real_product(first, second):
    return jnp.dot(first.astype(jnp.float32), second.astype(jnp.float32), precision=lax.Precision.HIGHEST, preferred_element_type=jnp.float32)

def complex_product(first, second):
    return (real_product(first[0], second[0]) - real_product(first[1], second[1]), real_product(first[0], second[1]) + real_product(first[1], second[0]))

def invert_exact(real_part, imag_part):
    orbitals = real_part.shape[0]
    stacked = jnp.concatenate([jnp.concatenate([real_part, -imag_part], axis=1), jnp.concatenate([imag_part, real_part], axis=1)], axis=0)
    whole = jnp.linalg.inv(stacked)
    return (whole[:orbitals, :orbitals], whole[orbitals:, :orbitals])

def reference(onsite_energy, onsite_mixing, hop_strength, hop_mixing, energy, broadening):
    orbitals = onsite_mixing.shape[1]
    identity = jnp.eye(orbitals, dtype=jnp.float32)
    hamilton = jax.vmap(jnp.diag)(onsite_energy) + 0.5 * (onsite_mixing + jnp.swapaxes(onsite_mixing, 1, 2))
    diagonal_real = energy[0] * identity - hamilton
    diagonal_imag = broadening[0] * identity
    couplings = jax.vmap(jnp.diag)(hop_strength) + hop_mixing
    empty_block = jnp.zeros((orbitals, orbitals), jnp.float32)

    def sweep_forward(carried, inputs):
        previous_real, previous_imag, coupling = carried
        block_real, next_coupling = inputs
        reduced_real = block_real - real_product(real_product(coupling.T, previous_real), coupling)
        reduced_imag = diagonal_imag - real_product(real_product(coupling.T, previous_imag), coupling)
        connected = invert_exact(reduced_real, reduced_imag)
        return ((connected[0], connected[1], next_coupling), connected)
    ending, connected = lax.scan(sweep_forward, (empty_block, empty_block, empty_block), (diagonal_real, couplings))

    def sweep_backward(following, inputs):
        here_real, here_imag, coupling = inputs
        left_side = (real_product(here_real, coupling), real_product(here_imag, coupling))
        middle = complex_product(left_side, following)
        right_side = (real_product(middle[0], coupling.T), real_product(middle[1], coupling.T))
        correction = complex_product(right_side, (here_real, here_imag))
        result = (here_real + correction[0], here_imag + correction[1])
        return (result, result)
    final_block = (connected[0][-1], connected[1][-1])
    leftover, earlier = lax.scan(sweep_backward, final_block, (connected[0][:-1], connected[1][:-1], couplings[:-1]), reverse=True)
    green_real = jnp.concatenate([earlier[0], final_block[0][None]], axis=0)
    green_imag = jnp.concatenate([earlier[1], final_block[1][None]], axis=0)
    return (green_real, green_imag)
```

```python
import functools

import jax
import jax.numpy as jnp
from jax import lax
from jax.experimental import pallas as pl
from jax.experimental.pallas import tpu as pltpu
from jax.sharding import PartitionSpec as P

MESH = pl.DeviceIdType.MESH
F32 = jnp.float32
STRIP = 8


def times(a, b):
    return a[0] * b[0] - a[1] * b[1], a[0] * b[1] + a[1] * b[0]


def minus(a, b):
    return a[0] - b[0], a[1] - b[1]


def select(mask, a, b):
    return jnp.where(mask, a[0], b[0]), jnp.where(mask, a[1], b[1])


def row_of(x, j):
    return tuple(jnp.broadcast_to(v[j : j + 1, :], v.shape) for v in x)


def lane_of(x, lanes):
    return tuple(jnp.take_along_axis(v, lanes, axis=1) for v in x)


def dot(a, b, transpose_b=False):
    dims = (((1,), (1 if transpose_b else 0,)), ((), ()))
    return lax.dot_general(a, b, dims, precision=lax.Precision.HIGHEST, preferred_element_type=F32)


def beside(x):
    return jnp.concatenate([x[0], x[1]], axis=1)


def square(x):
    top = jnp.concatenate([x[0], x[1]], axis=1)
    return jnp.concatenate([top, jnp.concatenate([-x[1], x[0]], axis=1)], axis=0)


def square_t(x):
    top = jnp.concatenate([x[0], -x[1]], axis=1)
    return jnp.concatenate([top, jnp.concatenate([x[1], x[0]], axis=1)], axis=0)


def halves(x):
    n = x.shape[1] // 2
    return x[:, :n], x[:, n:]


def cdot(a, b):
    return halves(dot(beside(a), square(b)))


def cdot_t(a, b):
    return halves(dot(beside(a), square_t(b), transpose_b=True))


def eliminated(rows, col_lanes, in_strip, sub, lane, first):
    columns = [lane_of(rows, lanes) for lanes in col_lanes]
    eye = jnp.where(lane - first == sub, 1.0, 0.0)
    rows = select(in_strip, (eye, jnp.zeros_like(eye)), rows)
    for j in range(STRIP):
        own = sub == j
        factor = columns[j]
        pivot = row_of(factor, j)
        scale = 1.0 / (pivot[0] * pivot[0] + pivot[1] * pivot[1])
        inverse = (pivot[0] * scale, -pivot[1] * scale)
        for k in range(j + 1, STRIP):
            entry = row_of(columns[k], j)
            columns[k] = select(
                own,
                times(entry, inverse),
                minus(columns[k], times(times(factor, entry), inverse)),
            )
        entry = row_of(rows, j)
        rows = select(
            own, times(entry, inverse), minus(rows, times(times(factor, inverse), entry))
        )
    return rows


def invert(mats):
    n = mats[0][0].shape[0]
    strips = n // STRIP
    lane = lax.broadcasted_iota(jnp.int32, (STRIP, n), 1)
    sub = lax.broadcasted_iota(jnp.int32, (STRIP, n), 0)
    zero = jnp.zeros((STRIP, n), F32)

    def lanes_of(step):
        return [jnp.full((STRIP, n), step * STRIP + j, jnp.int32) for j in range(STRIP)]

    def updated(x, lanes, in_strip, pivots):
        columns = [lane_of(x, ids) for ids in lanes]
        x = select(in_strip, (zero, zero), x)
        for j in range(STRIP):
            x = minus(x, times(columns[j], pivots[j]))
        return x

    def trail(mat, step, lanes, in_strip, strip, pivots):
        for i in range(strips):
            rows = slice(i * STRIP, (i + 1) * STRIP)
            x = updated((mat[0][rows, :], mat[1][rows, :]), lanes, in_strip, pivots)
            x = select(jnp.full((STRIP, n), i == step), strip, x)
            mat[0][rows, :] = x[0]
            mat[1][rows, :] = x[1]

    def body(step, carry):
        lanes_before, lanes = lanes_of(jnp.maximum(step - 1, 0)), lanes_of(step)
        in_before, in_strip = lane // STRIP == step - 1, lane // STRIP == step
        ahead = pl.multiple_of(jnp.minimum(step + 1, strips - 1) * STRIP, STRIP)
        out = []
        for mat, (rows, before) in zip(mats, carry):
            pivots = [row_of(before, j) for j in range(STRIP)]
            following = (mat[0][pl.ds(ahead, STRIP), :], mat[1][pl.ds(ahead, STRIP), :])
            following = updated(following, lanes_before, in_before, pivots)
            columns = [lane_of(following, ids) for ids in lanes]
            following = select(in_strip, (zero, zero), following)
            trail(mat, step - 1, lanes_before, in_before, before, pivots)
            rows = eliminated(rows, lanes, in_strip, sub, lane, step * STRIP)
            for j in range(STRIP):
                following = minus(following, times(columns[j], row_of(rows, j)))
            out.append((following, rows))
        return tuple(out)

    start = tuple(
        ((mat[0][0:STRIP, :], mat[1][0:STRIP, :]), (zero, zero)) for mat in mats
    )
    last = lax.fori_loop(0, strips, body, start)
    for mat, (_, strip) in zip(mats, last):
        pivots = [row_of(strip, j) for j in range(STRIP)]
        trail(mat, strips - 1, lanes_of(strips - 1), lane // STRIP == strips - 1, strip, pivots)


def packed(x, row, col):
    diagonal = jnp.sum(jnp.where(row == col, x[1], 0.0), axis=0, keepdims=True)
    mean = 0.5 * (jnp.where(row >= col, x[0], x[1]) + jnp.where(row <= col, x[0], x[1]).T)
    return mean, jnp.broadcast_to(diagonal, (STRIP, x[0].shape[1]))


def unpacked(ref, row, col):
    n = ref.shape[1]
    body = ref[0:n, :]
    other = body.T
    diagonal = jnp.broadcast_to(ref[n : n + 1, :], (n, n))
    real = jnp.where(row >= col, body, other)
    imag = jnp.where(row < col, body, jnp.where(row > col, other, diagonal))
    return real, imag


def kernel(
    count, onsite_ref, mixing_ref, strength_ref, hopping_ref, energy_ref, broadening_ref,
    real_ref, imag_ref,
    own_ref, low_ref, high_ref, work, spare,
    packed_out, packed_low, packed_high, link_low, link_high, from_low, from_high, strength_low,
    pack_up_send, pack_up_recv, pack_down_send, pack_down_recv,
    link_up_send, link_up_recv, link_down_send, link_down_recv, raw_send, raw_recv,
):
    levels = count.bit_length() - 1
    last = levels + 1
    n = mixing_ref.shape[1]
    me = lax.axis_index("slab")
    row = lax.broadcasted_iota(jnp.int32, (n, n), 0)
    col = lax.broadcasted_iota(jnp.int32, (n, n), 1)
    broadening = jnp.where(row == col, broadening_ref[0], 0.0)

    def diagonal(values):
        return jnp.where(row == col, jnp.broadcast_to(values, (n, n)), 0.0)

    def onsite(index):
        mixing = mixing_ref[index]
        hamilton = diagonal(onsite_ref[index : index + 1, :]) + 0.5 * (mixing + mixing.T)
        return jnp.where(row == col, energy_ref[0], 0.0) - hamilton

    def coupling(strengths, hoppings, index):
        return diagonal(strengths[index : index + 1, :]) + hoppings[index]

    def copy(source, target, send, recv, slab):
        return pltpu.make_async_remote_copy(
            src_ref=source, dst_ref=target, send_sem=send, recv_sem=recv,
            device_id={"slab": slab}, device_id_type=MESH,
        )

    def pack_up(slot, slab):
        return copy(packed_out.at[slot], packed_low.at[slot], pack_up_send.at[slot],
                    pack_up_recv.at[slot], slab)

    def pack_down(slot, slab):
        return copy(packed_out.at[slot], packed_high.at[slot], pack_down_send.at[slot],
                    pack_down_recv.at[slot], slab)

    def link_up(slot, slab):
        return copy(link_low.at[slot], from_low.at[slot], link_up_send.at[slot],
                    link_up_recv.at[slot], slab)

    def link_down(slot, slab):
        return copy(link_high.at[slot], from_high.at[slot], link_down_send.at[slot],
                    link_down_recv.at[slot], slab)

    def raw_mixing(slab):
        return copy(hopping_ref, from_low.at[0], raw_send.at[0], raw_recv.at[0], slab)

    def raw_strength(slab):
        return copy(strength_ref, strength_low, raw_send.at[1], raw_recv.at[1], slab)

    def pack(slot, value):
        square_part, tail_part = packed(value, row, col)
        packed_out[slot, 0:n, :] = square_part
        packed_out[slot, n : n + STRIP, :] = tail_part

    def set_work(refs, real):
        refs[0][...] = real
        refs[1][...] = broadening

    first = (work.at[0], work.at[1])
    second = (spare.at[0], spare.at[1])

    barrier = pltpu.get_barrier_semaphore()
    for level in range(levels):
        stride = 1 << level

        @pl.when(me >= stride)
        def _():
            pl.semaphore_signal(
                barrier, inc=1, device_id={"slab": me - stride}, device_id_type=MESH
            )

        @pl.when(me + stride < count)
        def _():
            pl.semaphore_signal(
                barrier, inc=1, device_id={"slab": me + stride}, device_id_type=MESH
            )

    peers = 0
    for level in range(levels):
        stride = 1 << level
        peers += (me >= stride).astype(jnp.int32) + (me + stride < count).astype(jnp.int32)
    pl.semaphore_wait(barrier, peers)

    @pl.when(me + 1 < count)
    def _():
        raw_mixing(me + 1).start()
        raw_strength(me + 1).start()

    @pl.when(me < 1)
    def _():
        from_low[0] = jnp.zeros((2, n, n), F32)
        strength_low[...] = jnp.zeros((2, n), F32)
        packed_low[0] = jnp.zeros((n + STRIP, n), F32)

    own_ref[...] = onsite(0)
    set_work(first, onsite(1))
    invert((first,))
    pack(0, (first[0][...], first[1][...]))

    @pl.when(me + 1 < count)
    def _():
        pack_up(0, me + 1).start()

    near = coupling(strength_ref, hopping_ref, 0)
    far = jnp.where(me < count - 1, coupling(strength_ref, hopping_ref, 1), 0.0)
    weight = halves(dot(near, beside(unpacked(packed_out.at[0], row, col))))
    both = jnp.concatenate([weight[0], weight[1]], axis=0)
    result = dot(both, near, transpose_b=True)
    high_ref[0] = result[:n]
    high_ref[1] = result[n:]
    result = dot(both, far)
    link_high[1, 0] = -result[:n]
    link_high[1, 1] = -result[n:]

    @pl.when(me >= 1)
    def _():
        raw_mixing(me).wait_recv()
        raw_strength(me).wait_recv()
        pack_up(0, me).wait_recv()

    near = coupling(strength_low, from_low.at[0], 0)
    far = coupling(strength_low, from_low.at[0], 1)
    weight = halves(dot(far.T, beside(unpacked(packed_low.at[0], row, col))))
    both = jnp.concatenate([weight[0], weight[1]], axis=0)
    result = dot(both, far)
    low_ref[0] = result[:n]
    low_ref[1] = result[n:]
    result = dot(both, near, transpose_b=True)
    link_low[1, 0] = -result[:n]
    link_low[1, 1] = -result[n:]

    def level_step(level, stride):
        has_low = me >= stride
        has_high = me + stride < count

        @pl.when(jnp.logical_and(level < levels, has_high))
        def _():
            link_up(level, me + stride).start()

        @pl.when(jnp.logical_and(level < levels, has_low))
        def _():
            link_down(level, me - stride).start()

        first[0][...] = own_ref[...] - low_ref[0] - high_ref[0]
        first[1][...] = broadening - low_ref[1] - high_ref[1]
        invert((first,))
        pack(level, (first[0][...], first[1][...]))

        @pl.when(has_high)
        def _():
            pack_up(level, me + stride).start()

        @pl.when(has_low)
        def _():
            pack_down(level, me - stride).start()

        @pl.when(jnp.logical_not(has_low))
        def _():
            from_low[level] = jnp.zeros((2, n, n), F32)
            packed_low[level] = jnp.zeros((n + STRIP, n), F32)

        @pl.when(jnp.logical_not(has_high))
        def _():
            from_high[level] = jnp.zeros((2, n, n), F32)
            packed_high[level] = jnp.zeros((n + STRIP, n), F32)

        @pl.when(has_low)
        def _():
            pack_up(level, me - stride).wait_recv()

        @pl.when(has_high)
        def _():
            pack_down(level, me + stride).wait_recv()

        low = (link_low[level, 0], link_low[level, 1])
        high = (link_high[level, 0], link_high[level, 1])
        low_weight = cdot(low, unpacked(packed_low.at[level], row, col))
        high_weight = cdot(high, unpacked(packed_high.at[level], row, col))
        term = cdot_t(low_weight, low)
        low_ref[0] += term[0]
        low_ref[1] += term[1]
        term = cdot_t(high_weight, high)
        high_ref[0] += term[0]
        high_ref[1] += term[1]

        @pl.when(level < levels)
        def _():
            @pl.when(has_low)
            def _():
                link_up(level, me - stride).wait_recv()

            @pl.when(has_high)
            def _():
                link_down(level, me + stride).wait_recv()

            term = cdot(low_weight, (from_low[level, 0], from_low[level, 1]))
            link_low[level + 1, 0] = -term[0]
            link_low[level + 1, 1] = -term[1]
            term = cdot(high_weight, (from_high[level, 0], from_high[level, 1]))
            link_high[level + 1, 0] = -term[0]
            link_high[level + 1, 1] = -term[1]

        return stride * 2

    lax.fori_loop(1, levels + 1, level_step, 1)

    first[0][...] = own_ref[...] - high_ref[0]
    first[1][...] = broadening - high_ref[1]
    second[0][...] = own_ref[...] - low_ref[0]
    second[1][...] = broadening - low_ref[1]
    invert((first, second))
    pack(last, (first[0][...], first[1][...]))

    @pl.when(me >= 1)
    def _():
        pack_down(last, me - 1).start()

    @pl.when(me + 1 >= count)
    def _():
        packed_high[last] = jnp.zeros((n + STRIP, n), F32)

    first[0][...] = own_ref[...] - low_ref[0] - high_ref[0]
    first[1][...] = broadening - low_ref[1] - high_ref[1]
    invert((first,))
    real_ref[0] = first[0][...]
    imag_ref[0] = first[1][...]

    near = coupling(strength_ref, hopping_ref, 0)
    far = jnp.where(me < count - 1, coupling(strength_ref, hopping_ref, 1), 0.0)
    mean = [0.5 * (ref[...] + ref[...].T) for ref in second]
    weight = halves(dot(near.T, beside(mean)))
    below = dot(jnp.concatenate([weight[0], weight[1]], axis=0), near)

    @pl.when(me + 1 < count)
    def _():
        pack_down(last, me + 1).wait_recv()

    weight = halves(dot(far, beside(unpacked(packed_high.at[last], row, col))))
    above = dot(jnp.concatenate([weight[0], weight[1]], axis=0), far, transpose_b=True)
    first[0][...] = onsite(1) - below[:n] - above[:n]
    first[1][...] = broadening - below[n:] - above[n:]
    invert((first,))
    real_ref[1] = first[0][...]
    imag_ref[1] = first[1][...]

    @pl.when(me + 1 < count)
    def _():
        raw_mixing(me + 1).wait_send()
        raw_strength(me + 1).wait_send()
        pack_up(0, me + 1).wait_send()

    @pl.when(me >= 1)
    def _():
        pack_down(last, me - 1).wait_send()

    def drain(level, stride):
        has_low = me >= stride
        has_high = me + stride < count

        @pl.when(has_high)
        def _():
            pack_up(level, me + stride).wait_send()

        @pl.when(has_low)
        def _():
            pack_down(level, me - stride).wait_send()

        @pl.when(jnp.logical_and(level < levels, has_high))
        def _():
            link_up(level, me + stride).wait_send()

        @pl.when(jnp.logical_and(level < levels, has_low))
        def _():
            link_down(level, me - stride).wait_send()

        return stride * 2

    lax.fori_loop(1, levels + 1, drain, 1)


def solution(mesh):
    count = mesh.shape["slab"]
    levels = count.bit_length() - 1

    def shards(onsite_energy, onsite_mixing, hop_strength, hop_mixing, energy, broadening):
        n = onsite_mixing.shape[1]
        whole = pl.BlockSpec(memory_space=pltpu.VMEM)
        scalar = pl.BlockSpec(memory_space=pltpu.SMEM)
        pair = jax.ShapeDtypeStruct((2, n, n), F32)
        pack_shape = pltpu.VMEM((levels + 2, n + STRIP, n), F32)
        link_shape = pltpu.VMEM((levels + 1, 2, n, n), F32)
        sems = pltpu.SemaphoreType.DMA((levels + 2,))
        return pl.pallas_call(
            functools.partial(kernel, count),
            out_shape=(pair, pair),
            in_specs=[whole] * 4 + [scalar] * 2,
            out_specs=(whole, whole),
            scratch_shapes=[
                pltpu.VMEM((n, n), F32),
                pltpu.VMEM((2, n, n), F32),
                pltpu.VMEM((2, n, n), F32),
                pltpu.VMEM((2, n, n), F32),
                pltpu.VMEM((2, n, n), F32),
                pack_shape, pack_shape, pack_shape,
                link_shape, link_shape, link_shape, link_shape,
                pltpu.VMEM((2, n), F32),
            ]
            + [sems] * 8
            + [pltpu.SemaphoreType.DMA((2,))] * 2,
            compiler_params=pltpu.CompilerParams(
                collective_id=0, has_side_effects=True, vmem_limit_bytes=40 * 1024 * 1024
            ),
        )(onsite_energy, onsite_mixing, hop_strength, hop_mixing, energy, broadening)

    return jax.shard_map(
        shards,
        mesh=mesh,
        in_specs=(
            P("slab", None),
            P("slab", None, None),
            P("slab", None),
            P("slab", None, None),
            P("energy"),
            P("energy"),
        ),
        out_specs=(P(("energy", "slab"), None, None), P(("energy", "slab"), None, None)),
        check_vma=False,
    )
```

```python
import functools

import jax
import jax.numpy as jnp
from jax import lax
from jax.experimental import pallas as pl
from jax.experimental.pallas import tpu as pltpu
from jax.sharding import PartitionSpec as P

MESH = pl.DeviceIdType.MESH
F32 = jnp.float32
STRIP = 8
PANEL = 32


def times(a, b):
    return a[0] * b[0] - a[1] * b[1], a[0] * b[1] + a[1] * b[0]


def minus(a, b):
    return a[0] - b[0], a[1] - b[1]


def select(mask, a, b):
    return jnp.where(mask, a[0], b[0]), jnp.where(mask, a[1], b[1])


def row_of(x, j):
    return tuple(jnp.broadcast_to(v[j : j + 1, :], v.shape) for v in x)


def lane_of(x, k):
    return tuple(jnp.broadcast_to(v[:, k : k + 1], v.shape) for v in x)


def dot(a, b, transpose_b=False):
    dims = (((1,), (1 if transpose_b else 0,)), ((), ()))
    return lax.dot_general(a, b, dims, precision=lax.Precision.HIGHEST, preferred_element_type=F32)


def beside(x):
    return jnp.concatenate([x[0], x[1]], axis=1)


def square(x):
    top = jnp.concatenate([x[0], x[1]], axis=1)
    return jnp.concatenate([top, jnp.concatenate([-x[1], x[0]], axis=1)], axis=0)


def square_t(x):
    top = jnp.concatenate([x[0], -x[1]], axis=1)
    return jnp.concatenate([top, jnp.concatenate([x[1], x[0]], axis=1)], axis=0)


def halves(x):
    n = x.shape[1] // 2
    return x[:, :n], x[:, n:]


def cdot(a, b):
    return halves(dot(beside(a), square(b)))


def cdot_t(a, b):
    return halves(dot(beside(a), square_t(b), transpose_b=True))


def eliminated(rows, columns, first, sub, lane):
    zero = jnp.zeros_like(rows[0])
    eye = jnp.where(lane - first == sub, 1.0, 0.0)
    rows = select((lane >= first) & (lane < first + STRIP), (eye, zero), rows)
    for j in range(STRIP):
        own = sub == j
        factor = columns[j]
        pivot = row_of(factor, j)
        scale = 1.0 / (pivot[0] * pivot[0] + pivot[1] * pivot[1])
        inverse = (pivot[0] * scale, -pivot[1] * scale)
        if j + 1 < STRIP:
            entry = row_of(columns[j + 1], j)
            change = select(own, (-entry[0], -entry[1]), times(factor, entry))
            columns[j + 1] = minus(
                select(own, (zero, zero), columns[j + 1]), times(change, inverse)
            )
        factor = select(own, (-inverse[0], -inverse[1]), times(factor, inverse))
        for k in range(j + 2, STRIP):
            change = times(factor, row_of(columns[k], j))
            columns[k] = minus(select(own, (zero, zero), columns[k]), change)
        rows = minus(select(own, (zero, zero), rows), times(factor, row_of(rows, j)))
    return rows


def swept(strips, start, sub, lane):
    zero = jnp.zeros_like(strips[0][0])
    count = len(strips)
    for s in range(count):
        first = start + s * STRIP
        columns = [[lane_of(x, first + j) for j in range(STRIP)] for x in strips]
        done = eliminated(strips[s], columns[s], first, sub, lane)
        pivots = [row_of(done, j) for j in range(STRIP)]
        here = (lane >= first) & (lane < first + STRIP)
        for step in range(1, count):
            i = (s + step) % count
            x = select(here, (zero, zero), strips[i])
            for j in range(STRIP):
                x = minus(x, times(columns[i][j], pivots[j]))
            strips[i] = x
        strips[s] = done
    return strips


def invert(mats):
    n = mats[0][0].shape[0]
    lane = lax.broadcasted_iota(jnp.int32, (STRIP, n), 1)
    sub = lax.broadcasted_iota(jnp.int32, (STRIP, n), 0)
    wide = lax.broadcasted_iota(jnp.int32, (n, n), 1)
    for start in range(0, n, PANEL):
        stop = start + PANEL
        here = (wide >= start) & (wide < stop)
        for mat in mats:
            strips = [tuple(r[a : a + STRIP, :] for r in mat) for a in range(start, stop, STRIP)]
            strips = swept(strips, start, sub, lane)
            panel = [jnp.concatenate([x[c] for x in strips], axis=0) for c in (0, 1)]
            left = jnp.concatenate([r[:, start:stop] for r in mat], axis=1)
            change = halves(dot(left, square(panel)))
            for c in (0, 1):
                mat[c][...] = jnp.where(here, 0.0, mat[c][...]) - change[c]
                mat[c][start:stop, :] = panel[c]


def packed(x, row, col):
    diagonal = jnp.sum(jnp.where(row == col, x[1], 0.0), axis=0, keepdims=True)
    mean = 0.5 * (jnp.where(row >= col, x[0], x[1]) + jnp.where(row <= col, x[0], x[1]).T)
    return mean, jnp.broadcast_to(diagonal, (STRIP, x[0].shape[1]))


def unpacked(ref, row, col):
    n = ref.shape[1]
    body = ref[0:n, :]
    other = body.T
    diagonal = jnp.broadcast_to(ref[n : n + 1, :], (n, n))
    real = jnp.where(row >= col, body, other)
    imag = jnp.where(row < col, body, jnp.where(row > col, other, diagonal))
    return real, imag


def kernel(
    count, onsite_ref, mixing_ref, strength_ref, hopping_ref, energy_ref, broadening_ref,
    real_ref, imag_ref,
    own_ref, low_ref, high_ref, work, spare,
    packed_out, packed_low, packed_high, link_low, link_high, from_low, from_high, strength_low,
    pack_up_send, pack_up_recv, pack_down_send, pack_down_recv,
    link_up_send, link_up_recv, link_down_send, link_down_recv, raw_send, raw_recv,
):
    levels = count.bit_length() - 1
    last = levels + 1
    n = mixing_ref.shape[1]
    me = lax.axis_index("slab")
    row = lax.broadcasted_iota(jnp.int32, (n, n), 0)
    col = lax.broadcasted_iota(jnp.int32, (n, n), 1)
    broadening = jnp.where(row == col, broadening_ref[0], 0.0)

    def diagonal(values):
        return jnp.where(row == col, jnp.broadcast_to(values, (n, n)), 0.0)

    def onsite(index):
        mixing = mixing_ref[index]
        hamilton = diagonal(onsite_ref[index : index + 1, :]) + 0.5 * (mixing + mixing.T)
        return jnp.where(row == col, energy_ref[0], 0.0) - hamilton

    def coupling(strengths, hoppings, index):
        return diagonal(strengths[index : index + 1, :]) + hoppings[index]

    def copy(source, target, send, recv, slab):
        return pltpu.make_async_remote_copy(
            src_ref=source, dst_ref=target, send_sem=send, recv_sem=recv,
            device_id={"slab": slab}, device_id_type=MESH,
        )

    def pack_up(slot, slab):
        return copy(packed_out.at[slot], packed_low.at[slot], pack_up_send.at[slot],
                    pack_up_recv.at[slot], slab)

    def pack_down(slot, slab):
        return copy(packed_out.at[slot], packed_high.at[slot], pack_down_send.at[slot],
                    pack_down_recv.at[slot], slab)

    def link_up(slot, slab):
        return copy(link_low.at[slot], from_low.at[slot], link_up_send.at[slot],
                    link_up_recv.at[slot], slab)

    def link_down(slot, slab):
        return copy(link_high.at[slot], from_high.at[slot], link_down_send.at[slot],
                    link_down_recv.at[slot], slab)

    def raw_mixing(slab):
        return copy(hopping_ref, from_low.at[0], raw_send.at[0], raw_recv.at[0], slab)

    def raw_strength(slab):
        return copy(strength_ref, strength_low, raw_send.at[1], raw_recv.at[1], slab)

    def pack(slot, value):
        square_part, tail_part = packed(value, row, col)
        packed_out[slot, 0:n, :] = square_part
        packed_out[slot, n : n + STRIP, :] = tail_part

    def set_work(refs, real):
        refs[0][...] = real
        refs[1][...] = broadening

    first = (work.at[0], work.at[1])
    second = (spare.at[0], spare.at[1])

    barrier = pltpu.get_barrier_semaphore()
    for level in range(levels):
        stride = 1 << level

        @pl.when(me >= stride)
        def _():
            pl.semaphore_signal(
                barrier, inc=1, device_id={"slab": me - stride}, device_id_type=MESH
            )

        @pl.when(me + stride < count)
        def _():
            pl.semaphore_signal(
                barrier, inc=1, device_id={"slab": me + stride}, device_id_type=MESH
            )

    peers = 0
    for level in range(levels):
        stride = 1 << level
        peers += (me >= stride).astype(jnp.int32) + (me + stride < count).astype(jnp.int32)
    pl.semaphore_wait(barrier, peers)

    @pl.when(me + 1 < count)
    def _():
        raw_mixing(me + 1).start()
        raw_strength(me + 1).start()

    @pl.when(me < 1)
    def _():
        from_low[0] = jnp.zeros((2, n, n), F32)
        strength_low[...] = jnp.zeros((2, n), F32)
        packed_low[0] = jnp.zeros((n + STRIP, n), F32)

    own_ref[...] = onsite(0)
    set_work(first, onsite(1))
    invert((first,))
    pack(0, (first[0][...], first[1][...]))

    @pl.when(me + 1 < count)
    def _():
        pack_up(0, me + 1).start()

    near = coupling(strength_ref, hopping_ref, 0)
    far = jnp.where(me < count - 1, coupling(strength_ref, hopping_ref, 1), 0.0)
    weight = halves(dot(near, beside(unpacked(packed_out.at[0], row, col))))
    both = jnp.concatenate([weight[0], weight[1]], axis=0)
    result = dot(both, near, transpose_b=True)
    high_ref[0] = result[:n]
    high_ref[1] = result[n:]
    result = dot(both, far)
    link_high[1, 0] = -result[:n]
    link_high[1, 1] = -result[n:]

    @pl.when(me >= 1)
    def _():
        raw_mixing(me).wait_recv()
        raw_strength(me).wait_recv()
        pack_up(0, me).wait_recv()

    near = coupling(strength_low, from_low.at[0], 0)
    far = coupling(strength_low, from_low.at[0], 1)
    weight = halves(dot(far.T, beside(unpacked(packed_low.at[0], row, col))))
    both = jnp.concatenate([weight[0], weight[1]], axis=0)
    result = dot(both, far)
    low_ref[0] = result[:n]
    low_ref[1] = result[n:]
    result = dot(both, near, transpose_b=True)
    link_low[1, 0] = -result[:n]
    link_low[1, 1] = -result[n:]

    def level_step(level, stride):
        has_low = me >= stride
        has_high = me + stride < count

        @pl.when(jnp.logical_and(level < levels, has_high))
        def _():
            link_up(level, me + stride).start()

        @pl.when(jnp.logical_and(level < levels, has_low))
        def _():
            link_down(level, me - stride).start()

        first[0][...] = own_ref[...] - low_ref[0] - high_ref[0]
        first[1][...] = broadening - low_ref[1] - high_ref[1]
        invert((first,))
        pack(level, (first[0][...], first[1][...]))

        @pl.when(has_high)
        def _():
            pack_up(level, me + stride).start()

        @pl.when(has_low)
        def _():
            pack_down(level, me - stride).start()

        @pl.when(jnp.logical_not(has_low))
        def _():
            from_low[level] = jnp.zeros((2, n, n), F32)
            packed_low[level] = jnp.zeros((n + STRIP, n), F32)

        @pl.when(jnp.logical_not(has_high))
        def _():
            from_high[level] = jnp.zeros((2, n, n), F32)
            packed_high[level] = jnp.zeros((n + STRIP, n), F32)

        @pl.when(has_low)
        def _():
            pack_up(level, me - stride).wait_recv()

        @pl.when(has_high)
        def _():
            pack_down(level, me + stride).wait_recv()

        low = (link_low[level, 0], link_low[level, 1])
        high = (link_high[level, 0], link_high[level, 1])
        low_weight = cdot(low, unpacked(packed_low.at[level], row, col))
        high_weight = cdot(high, unpacked(packed_high.at[level], row, col))
        term = cdot_t(low_weight, low)
        low_ref[0] += term[0]
        low_ref[1] += term[1]
        term = cdot_t(high_weight, high)
        high_ref[0] += term[0]
        high_ref[1] += term[1]

        @pl.when(level < levels)
        def _():
            @pl.when(has_low)
            def _():
                link_up(level, me - stride).wait_recv()

            @pl.when(has_high)
            def _():
                link_down(level, me + stride).wait_recv()

            term = cdot(low_weight, (from_low[level, 0], from_low[level, 1]))
            link_low[level + 1, 0] = -term[0]
            link_low[level + 1, 1] = -term[1]
            term = cdot(high_weight, (from_high[level, 0], from_high[level, 1]))
            link_high[level + 1, 0] = -term[0]
            link_high[level + 1, 1] = -term[1]

        return stride * 2

    lax.fori_loop(1, levels + 1, level_step, 1)

    first[0][...] = own_ref[...] - high_ref[0]
    first[1][...] = broadening - high_ref[1]
    second[0][...] = own_ref[...] - low_ref[0]
    second[1][...] = broadening - low_ref[1]
    invert((first, second))
    pack(last, (first[0][...], first[1][...]))

    @pl.when(me >= 1)
    def _():
        pack_down(last, me - 1).start()

    @pl.when(me + 1 >= count)
    def _():
        packed_high[last] = jnp.zeros((n + STRIP, n), F32)

    first[0][...] = own_ref[...] - low_ref[0] - high_ref[0]
    first[1][...] = broadening - low_ref[1] - high_ref[1]
    invert((first,))
    real_ref[0] = first[0][...]
    imag_ref[0] = first[1][...]

    near = coupling(strength_ref, hopping_ref, 0)
    far = jnp.where(me < count - 1, coupling(strength_ref, hopping_ref, 1), 0.0)
    mean = [0.5 * (ref[...] + ref[...].T) for ref in second]
    weight = halves(dot(near.T, beside(mean)))
    below = dot(jnp.concatenate([weight[0], weight[1]], axis=0), near)

    @pl.when(me + 1 < count)
    def _():
        pack_down(last, me + 1).wait_recv()

    weight = halves(dot(far, beside(unpacked(packed_high.at[last], row, col))))
    above = dot(jnp.concatenate([weight[0], weight[1]], axis=0), far, transpose_b=True)
    first[0][...] = onsite(1) - below[:n] - above[:n]
    first[1][...] = broadening - below[n:] - above[n:]
    invert((first,))
    real_ref[1] = first[0][...]
    imag_ref[1] = first[1][...]

    @pl.when(me + 1 < count)
    def _():
        raw_mixing(me + 1).wait_send()
        raw_strength(me + 1).wait_send()
        pack_up(0, me + 1).wait_send()

    @pl.when(me >= 1)
    def _():
        pack_down(last, me - 1).wait_send()

    def drain(level, stride):
        has_low = me >= stride
        has_high = me + stride < count

        @pl.when(has_high)
        def _():
            pack_up(level, me + stride).wait_send()

        @pl.when(has_low)
        def _():
            pack_down(level, me - stride).wait_send()

        @pl.when(jnp.logical_and(level < levels, has_high))
        def _():
            link_up(level, me + stride).wait_send()

        @pl.when(jnp.logical_and(level < levels, has_low))
        def _():
            link_down(level, me - stride).wait_send()

        return stride * 2

    lax.fori_loop(1, levels + 1, drain, 1)


def solution(mesh):
    count = mesh.shape["slab"]
    levels = count.bit_length() - 1

    def shards(onsite_energy, onsite_mixing, hop_strength, hop_mixing, energy, broadening):
        n = onsite_mixing.shape[1]
        whole = pl.BlockSpec(memory_space=pltpu.VMEM)
        scalar = pl.BlockSpec(memory_space=pltpu.SMEM)
        pair = jax.ShapeDtypeStruct((2, n, n), F32)
        pack_shape = pltpu.VMEM((levels + 2, n + STRIP, n), F32)
        link_shape = pltpu.VMEM((levels + 1, 2, n, n), F32)
        sems = pltpu.SemaphoreType.DMA((levels + 2,))
        return pl.pallas_call(
            functools.partial(kernel, count),
            out_shape=(pair, pair),
            in_specs=[whole] * 4 + [scalar] * 2,
            out_specs=(whole, whole),
            scratch_shapes=[
                pltpu.VMEM((n, n), F32),
                pltpu.VMEM((2, n, n), F32),
                pltpu.VMEM((2, n, n), F32),
                pltpu.VMEM((2, n, n), F32),
                pltpu.VMEM((2, n, n), F32),
                pack_shape, pack_shape, pack_shape,
                link_shape, link_shape, link_shape, link_shape,
                pltpu.VMEM((2, n), F32),
            ]
            + [sems] * 8
            + [pltpu.SemaphoreType.DMA((2,))] * 2,
            compiler_params=pltpu.CompilerParams(
                collective_id=0, has_side_effects=True, vmem_limit_bytes=40 * 1024 * 1024
            ),
        )(onsite_energy, onsite_mixing, hop_strength, hop_mixing, energy, broadening)

    return jax.shard_map(
        shards,
        mesh=mesh,
        in_specs=(
            P("slab", None),
            P("slab", None, None),
            P("slab", None),
            P("slab", None, None),
            P("energy"),
            P("energy"),
        ),
        out_specs=(P(("energy", "slab"), None, None), P(("energy", "slab"), None, None)),
        check_vma=False,
    )
```

```python
import functools

import jax
import jax.numpy as jnp
from jax import lax
from jax.experimental import pallas as pl
from jax.experimental.pallas import tpu as pltpu
from jax.sharding import PartitionSpec as P

MESH = pl.DeviceIdType.MESH
F32 = jnp.float32
STRIP = 8
PANEL = 32


def times(a, b):
    return a[0] * b[0] - a[1] * b[1], a[0] * b[1] + a[1] * b[0]


def minus(a, b):
    return a[0] - b[0], a[1] - b[1]


def select(mask, a, b):
    return jnp.where(mask, a[0], b[0]), jnp.where(mask, a[1], b[1])


def row_of(x, j):
    return tuple(jnp.broadcast_to(v[j : j + 1, :], v.shape) for v in x)


def lane_of(x, k):
    lanes = jnp.full(x[0].shape, k, jnp.int32)
    return tuple(jnp.take_along_axis(v, lanes, axis=1) for v in x)


def dot(a, b, transpose_b=False):
    dims = (((1,), (1 if transpose_b else 0,)), ((), ()))
    return lax.dot_general(a, b, dims, precision=lax.Precision.HIGHEST, preferred_element_type=F32)


def beside(x):
    return jnp.concatenate([x[0], x[1]], axis=1)


def square(x):
    top = jnp.concatenate([x[0], x[1]], axis=1)
    return jnp.concatenate([top, jnp.concatenate([-x[1], x[0]], axis=1)], axis=0)


def square_t(x):
    top = jnp.concatenate([x[0], -x[1]], axis=1)
    return jnp.concatenate([top, jnp.concatenate([x[1], x[0]], axis=1)], axis=0)


def halves(x):
    n = x.shape[1] // 2
    return x[:, :n], x[:, n:]


def cdot(a, b):
    return halves(dot(beside(a), square(b)))


def cdot_t(a, b):
    return halves(dot(beside(a), square_t(b), transpose_b=True))


def eliminated(rows, columns, first, sub, lane):
    zero = jnp.zeros_like(rows[0])
    eye = jnp.where(lane - first == sub, 1.0, 0.0)
    rows = select((lane >= first) & (lane < first + STRIP), (eye, zero), rows)
    for j in range(STRIP):
        own = sub == j
        factor = columns[j]
        pivot = row_of(factor, j)
        scale = 1.0 / (pivot[0] * pivot[0] + pivot[1] * pivot[1])
        inverse = (pivot[0] * scale, -pivot[1] * scale)
        if j + 1 < STRIP:
            entry = row_of(columns[j + 1], j)
            change = select(own, (-entry[0], -entry[1]), times(factor, entry))
            columns[j + 1] = minus(
                select(own, (zero, zero), columns[j + 1]), times(change, inverse)
            )
        factor = select(own, (-inverse[0], -inverse[1]), times(factor, inverse))
        for k in range(j + 2, STRIP):
            change = times(factor, row_of(columns[k], j))
            columns[k] = minus(select(own, (zero, zero), columns[k]), change)
        rows = minus(select(own, (zero, zero), rows), times(factor, row_of(rows, j)))
    return rows


def swept(strips, start, sub, lane):
    zero = jnp.zeros_like(strips[0][0])
    count = len(strips)
    for s in range(count):
        first = start + s * STRIP
        columns = [[lane_of(x, first + j) for j in range(STRIP)] for x in strips]
        done = eliminated(strips[s], columns[s], first, sub, lane)
        pivots = [row_of(done, j) for j in range(STRIP)]
        here = (lane >= first) & (lane < first + STRIP)
        for step in range(1, count):
            i = (s + step) % count
            x = select(here, (zero, zero), strips[i])
            for j in range(STRIP):
                x = minus(x, times(columns[i][j], pivots[j]))
            strips[i] = x
        strips[s] = done
    return strips


def thirds(x):
    high = x.astype(jnp.bfloat16)
    rest = x - high.astype(F32)
    middle = rest.astype(jnp.bfloat16)
    return high, middle, (rest - middle.astype(F32)).astype(jnp.bfloat16)


def invert(mats):
    n = mats[0][0].shape[0]
    lane = lax.broadcasted_iota(jnp.int32, (STRIP, n), 1)
    sub = lax.broadcasted_iota(jnp.int32, (STRIP, n), 0)
    wide = lax.broadcasted_iota(jnp.int32, (n, n), 1)
    pair = wide < 2 * PANEL
    even = wide % (2 * PANEL) < PANEL

    def body(step, carry):
        start = pl.multiple_of(step * PANEL, PANEL)
        here = (wide >= start) & (wide < start + PANEL)
        for mat in mats:
            panel = tuple(r[pl.ds(start, PANEL), :] for r in mat)
            strips = [tuple(v[a : a + STRIP, :] for v in panel) for a in range(0, PANEL, STRIP)]
            moved = [
                pltpu.roll(mat[turn % 2][...], n - start + turn * PANEL, 1) for turn in range(4)
            ]
            left = jnp.where(
                pair, jnp.where(even, moved[0], moved[1]), jnp.where(even, moved[2], moved[3])
            )
            high, middle, low = thirds(left)
            left = jnp.concatenate(
                [high, jnp.where(pair, high, middle), jnp.where(pair, middle, low)], axis=1
            )
            strips = swept(strips, start, sub, lane)
            panel = [jnp.concatenate([x[c] for x in strips], axis=0) for c in (0, 1)]
            high, middle, low = thirds(square(panel))
            right = jnp.concatenate([high, middle, low, high, middle, high], axis=0)
            change = halves(jnp.dot(left, right, preferred_element_type=F32))
            for c in (0, 1):
                mat[c][...] = jnp.where(here, 0.0, mat[c][...]) - change[c]
                mat[c][pl.ds(start, PANEL), :] = panel[c]
        return carry

    lax.fori_loop(0, n // PANEL, body, 0)


def packed(x, row, col):
    diagonal = jnp.sum(jnp.where(row == col, x[1], 0.0), axis=0, keepdims=True)
    mean = 0.5 * (jnp.where(row >= col, x[0], x[1]) + jnp.where(row <= col, x[0], x[1]).T)
    return mean, jnp.broadcast_to(diagonal, (STRIP, x[0].shape[1]))


def unpacked(ref, row, col):
    n = ref.shape[1]
    body = ref[0:n, :]
    other = body.T
    diagonal = jnp.broadcast_to(ref[n : n + 1, :], (n, n))
    real = jnp.where(row >= col, body, other)
    imag = jnp.where(row < col, body, jnp.where(row > col, other, diagonal))
    return real, imag


def kernel(
    count, onsite_ref, mixing_ref, strength_ref, hopping_ref, energy_ref, broadening_ref,
    real_ref, imag_ref,
    own_ref, low_ref, high_ref, work, spare, weight_low, weight_high,
    packed_out, packed_low, packed_high, link_low, link_high, from_low, from_high, strength_low,
    pack_up_send, pack_up_recv, pack_down_send, pack_down_recv,
    link_up_send, link_up_recv, link_down_send, link_down_recv, raw_send, raw_recv,
):
    levels = count.bit_length() - 1
    last = levels + 1
    n = mixing_ref.shape[1]
    me = lax.axis_index("slab")
    row = lax.broadcasted_iota(jnp.int32, (n, n), 0)
    col = lax.broadcasted_iota(jnp.int32, (n, n), 1)
    broadening = jnp.where(row == col, broadening_ref[0], 0.0)

    def diagonal(values):
        return jnp.where(row == col, jnp.broadcast_to(values, (n, n)), 0.0)

    def onsite(index):
        mixing = mixing_ref[index]
        hamilton = diagonal(onsite_ref[index : index + 1, :]) + 0.5 * (mixing + mixing.T)
        return jnp.where(row == col, energy_ref[0], 0.0) - hamilton

    def coupling(strengths, hoppings, index):
        return diagonal(strengths[index : index + 1, :]) + hoppings[index]

    def copy(source, target, send, recv, slab):
        return pltpu.make_async_remote_copy(
            src_ref=source, dst_ref=target, send_sem=send, recv_sem=recv,
            device_id={"slab": slab}, device_id_type=MESH,
        )

    def pack_up(slot, slab):
        return copy(packed_out.at[slot], packed_low.at[slot], pack_up_send.at[slot],
                    pack_up_recv.at[slot], slab)

    def pack_down(slot, slab):
        return copy(packed_out.at[slot], packed_high.at[slot], pack_down_send.at[slot],
                    pack_down_recv.at[slot], slab)

    def link_up(slot, slab):
        return copy(link_low.at[slot], from_low.at[slot], link_up_send.at[slot],
                    link_up_recv.at[slot], slab)

    def link_down(slot, slab):
        return copy(link_high.at[slot], from_high.at[slot], link_down_send.at[slot],
                    link_down_recv.at[slot], slab)

    def raw_mixing(slab):
        return copy(hopping_ref, from_low.at[0], raw_send.at[0], raw_recv.at[0], slab)

    def raw_strength(slab):
        return copy(strength_ref, strength_low, raw_send.at[1], raw_recv.at[1], slab)

    def pack(slot, value):
        square_part, tail_part = packed(value, row, col)
        packed_out[slot, 0:n, :] = square_part
        packed_out[slot, n : n + STRIP, :] = tail_part

    def set_work(refs, real):
        refs[0][...] = real
        refs[1][...] = broadening

    def keep(ref, wide_value, sign=None):
        for c, value in enumerate(halves(wide_value)):
            ref[c] = value if sign is None else sign * value

    def add(ref, wide_value):
        for c, value in enumerate(halves(wide_value)):
            ref[c] += value

    def stacked(wide_value):
        return jnp.concatenate(halves(wide_value), axis=0)

    def side_by_side(tall_value):
        return jnp.concatenate([tall_value[:n], tall_value[n:]], axis=1)

    first = (work.at[0], work.at[1])
    second = (spare.at[0], spare.at[1])

    barrier = pltpu.get_barrier_semaphore()
    for level in range(levels):
        stride = 1 << level

        @pl.when(me >= stride)
        def _():
            pl.semaphore_signal(
                barrier, inc=1, device_id={"slab": me - stride}, device_id_type=MESH
            )

        @pl.when(me + stride < count)
        def _():
            pl.semaphore_signal(
                barrier, inc=1, device_id={"slab": me + stride}, device_id_type=MESH
            )

    peers = 0
    for level in range(levels):
        stride = 1 << level
        peers += (me >= stride).astype(jnp.int32) + (me + stride < count).astype(jnp.int32)
    pl.semaphore_wait(barrier, peers)

    @pl.when(me + 1 < count)
    def _():
        raw_mixing(me + 1).start()
        raw_strength(me + 1).start()

    @pl.when(me < 1)
    def _():
        from_low[0] = jnp.zeros((2, n, n), F32)
        strength_low[...] = jnp.zeros((2, n), F32)
        packed_low[0] = jnp.zeros((n + STRIP, n), F32)

    own_ref[...] = onsite(0)
    set_work(first, onsite(1))
    invert((first,))
    pack(0, (first[0][...], first[1][...]))

    @pl.when(me + 1 < count)
    def _():
        pack_up(0, me + 1).start()

    near = coupling(strength_ref, hopping_ref, 0)
    far = jnp.where(me < count - 1, coupling(strength_ref, hopping_ref, 1), 0.0)
    weight = dot(near, beside(unpacked(packed_out.at[0], row, col)))
    keep(weight_high, weight, -1.0)
    keep(high_ref, side_by_side(dot(stacked(weight), near, transpose_b=True)))
    from_high[0, 0] = -far
    from_high[0, 1] = jnp.zeros((n, n), F32)

    @pl.when(me >= 1)
    def _():
        raw_mixing(me).wait_recv()
        raw_strength(me).wait_recv()
        pack_up(0, me).wait_recv()

    near = coupling(strength_low, from_low.at[0], 0)
    far = coupling(strength_low, from_low.at[0], 1)
    weight = dot(far.T, beside(unpacked(packed_low.at[0], row, col)))
    keep(weight_low, weight, -1.0)
    keep(low_ref, side_by_side(dot(stacked(weight), far)))
    from_low[0, 0] = -near.T
    from_low[0, 1] = jnp.zeros((n, n), F32)

    def level_step(level, stride):
        has_low = me >= stride
        has_high = me + stride < count
        inner = jnp.logical_and(has_low, has_high)
        before = level - 1

        first[0][...] = own_ref[...] - low_ref[0] - high_ref[0]
        first[1][...] = broadening - low_ref[1] - high_ref[1]
        invert((first,))
        pack(level, (first[0][...], first[1][...]))

        @pl.when(has_high)
        def _():
            pack_up(level, me + stride).start()

        @pl.when(has_low)
        def _():
            pack_down(level, me - stride).start()

        @pl.when(jnp.logical_and(level > 1, has_low))
        def _():
            link_up(before, me - stride // 2).wait_recv()

        @pl.when(jnp.logical_and(level > 1, has_high))
        def _():
            link_down(before, me + stride // 2).wait_recv()

        @pl.when(jnp.logical_not(has_low))
        def _():
            from_low[before] = jnp.zeros((2, n, n), F32)
            packed_low[level] = jnp.zeros((n + STRIP, n), F32)

        @pl.when(jnp.logical_not(has_high))
        def _():
            from_high[before] = jnp.zeros((2, n, n), F32)
            packed_high[level] = jnp.zeros((n + STRIP, n), F32)

        low = (from_low[before, 0], from_low[before, 1])
        low = dot(beside((weight_low[0], weight_low[1])), square(low))
        keep(link_low.at[level], low, -1.0)
        high = (from_high[before, 0], from_high[before, 1])
        high = dot(beside((weight_high[0], weight_high[1])), square(high))
        keep(link_high.at[level], high, -1.0)

        @pl.when(inner)
        def _():
            link_up(level, me + stride).start()
            link_down(level, me - stride).start()

        @pl.when(has_low)
        def _():
            pack_up(level, me - stride).wait_recv()

        @pl.when(has_high)
        def _():
            pack_down(level, me + stride).wait_recv()

        low = (link_low[level, 0], link_low[level, 1])
        high = (link_high[level, 0], link_high[level, 1])
        low_weight = dot(beside(low), square(unpacked(packed_low.at[level], row, col)))
        high_weight = dot(beside(high), square(unpacked(packed_high.at[level], row, col)))
        keep(weight_low, low_weight)
        keep(weight_high, high_weight)
        add(low_ref, dot(low_weight, square_t(low), transpose_b=True))
        add(high_ref, dot(high_weight, square_t(high), transpose_b=True))
        return stride * 2

    lax.fori_loop(1, levels + 1, level_step, 1)

    first[0][...] = own_ref[...] - high_ref[0]
    first[1][...] = broadening - high_ref[1]
    second[0][...] = own_ref[...] - low_ref[0]
    second[1][...] = broadening - low_ref[1]
    invert((first, second))
    pack(last, (first[0][...], first[1][...]))

    @pl.when(me >= 1)
    def _():
        pack_down(last, me - 1).start()

    @pl.when(me + 1 >= count)
    def _():
        packed_high[last] = jnp.zeros((n + STRIP, n), F32)

    first[0][...] = own_ref[...] - low_ref[0] - high_ref[0]
    first[1][...] = broadening - low_ref[1] - high_ref[1]
    invert((first,))
    real_ref[0] = first[0][...]
    imag_ref[0] = first[1][...]

    near = coupling(strength_ref, hopping_ref, 0)
    far = jnp.where(me < count - 1, coupling(strength_ref, hopping_ref, 1), 0.0)
    mean = [0.5 * (ref[...] + ref[...].T) for ref in second]
    weight = halves(dot(near.T, beside(mean)))
    below = dot(jnp.concatenate([weight[0], weight[1]], axis=0), near)

    @pl.when(me + 1 < count)
    def _():
        pack_down(last, me + 1).wait_recv()

    weight = halves(dot(far, beside(unpacked(packed_high.at[last], row, col))))
    above = dot(jnp.concatenate([weight[0], weight[1]], axis=0), far, transpose_b=True)
    first[0][...] = onsite(1) - below[:n] - above[:n]
    first[1][...] = broadening - below[n:] - above[n:]
    invert((first,))
    real_ref[1] = first[0][...]
    imag_ref[1] = first[1][...]

    @pl.when(me + 1 < count)
    def _():
        raw_mixing(me + 1).wait_send()
        raw_strength(me + 1).wait_send()
        pack_up(0, me + 1).wait_send()

    @pl.when(me >= 1)
    def _():
        pack_down(last, me - 1).wait_send()

    def drain(level, stride):
        has_low = me >= stride
        has_high = me + stride < count

        @pl.when(has_high)
        def _():
            pack_up(level, me + stride).wait_send()

        @pl.when(has_low)
        def _():
            pack_down(level, me - stride).wait_send()

        @pl.when(jnp.logical_and(has_low, has_high))
        def _():
            link_up(level, me + stride).wait_send()
            link_down(level, me - stride).wait_send()

        return stride * 2

    lax.fori_loop(1, levels + 1, drain, 1)


def solution(mesh):
    count = mesh.shape["slab"]
    levels = count.bit_length() - 1

    def shards(onsite_energy, onsite_mixing, hop_strength, hop_mixing, energy, broadening):
        n = onsite_mixing.shape[1]
        whole = pl.BlockSpec(memory_space=pltpu.VMEM)
        scalar = pl.BlockSpec(memory_space=pltpu.SMEM)
        pair = jax.ShapeDtypeStruct((2, n, n), F32)
        pack_shape = pltpu.VMEM((levels + 2, n + STRIP, n), F32)
        link_shape = pltpu.VMEM((levels + 1, 2, n, n), F32)
        sems = pltpu.SemaphoreType.DMA((levels + 2,))
        return pl.pallas_call(
            functools.partial(kernel, count),
            out_shape=(pair, pair),
            in_specs=[whole] * 4 + [scalar] * 2,
            out_specs=(whole, whole),
            scratch_shapes=[
                pltpu.VMEM((n, n), F32),
                pltpu.VMEM((2, n, n), F32),
                pltpu.VMEM((2, n, n), F32),
                pltpu.VMEM((2, n, n), F32),
                pltpu.VMEM((2, n, n), F32),
                pltpu.VMEM((2, n, n), F32),
                pltpu.VMEM((2, n, n), F32),
                pack_shape, pack_shape, pack_shape,
                link_shape, link_shape, link_shape, link_shape,
                pltpu.VMEM((2, n), F32),
            ]
            + [sems] * 8
            + [pltpu.SemaphoreType.DMA((2,))] * 2,
            compiler_params=pltpu.CompilerParams(
                collective_id=0, has_side_effects=True, vmem_limit_bytes=40 * 1024 * 1024
            ),
        )(onsite_energy, onsite_mixing, hop_strength, hop_mixing, energy, broadening)

    return jax.shard_map(
        shards,
        mesh=mesh,
        in_specs=(
            P("slab", None),
            P("slab", None, None),
            P("slab", None),
            P("slab", None, None),
            P("energy"),
            P("energy"),
        ),
        out_specs=(P(("energy", "slab"), None, None), P(("energy", "slab"), None, None)),
        check_vma=False,
    )
```

```python
import functools

import jax
import jax.numpy as jnp
from jax import lax
from jax.experimental import pallas as pl
from jax.experimental.pallas import tpu as pltpu
from jax.sharding import PartitionSpec as P

MESH = pl.DeviceIdType.MESH
F32 = jnp.float32
STRIP = 8
PANEL = 32


def times(a, b):
    return a[0] * b[0] - a[1] * b[1], a[0] * b[1] + a[1] * b[0]


def plus(a, b):
    return a[0] + b[0], a[1] + b[1]


def minus(a, b):
    return a[0] - b[0], a[1] - b[1]


def select(mask, a, b):
    return jnp.where(mask, a[0], b[0]), jnp.where(mask, a[1], b[1])


def row_of(x, j):
    return tuple(jnp.broadcast_to(v[j : j + 1, :], v.shape) for v in x)


def lane_of(x, k):
    lanes = jnp.full(x[0].shape, k, jnp.int32)
    return tuple(jnp.take_along_axis(v, lanes, axis=1) for v in x)


def dot(a, b, transpose_b=False):
    dims = (((1,), (1 if transpose_b else 0,)), ((), ()))
    return lax.dot_general(a, b, dims, precision=lax.Precision.HIGHEST, preferred_element_type=F32)


def beside(x):
    return jnp.concatenate([x[0], x[1]], axis=1)


def square(x):
    top = jnp.concatenate([x[0], x[1]], axis=1)
    return jnp.concatenate([top, jnp.concatenate([-x[1], x[0]], axis=1)], axis=0)


def square_t(x):
    top = jnp.concatenate([x[0], -x[1]], axis=1)
    return jnp.concatenate([top, jnp.concatenate([x[1], x[0]], axis=1)], axis=0)


def halves(x):
    n = x.shape[1] // 2
    return x[:, :n], x[:, n:]


def cdot(a, b):
    return halves(dot(beside(a), square(b)))


def cdot_t(a, b):
    return halves(dot(beside(a), square_t(b), transpose_b=True))


def eliminated(rows, columns, first, sub, lane):
    zero = jnp.zeros_like(rows[0])
    none = (zero, zero)
    eye = jnp.where(lane - first == sub, 1.0, 0.0)
    rows = select((lane >= first) & (lane < first + STRIP), (eye, zero), rows)
    for j in range(0, STRIP, 2):
        top, bottom = sub == j, sub == j + 1
        own = top | bottom
        f, g = columns[j], columns[j + 1]
        a, c = row_of(f, j), row_of(f, j + 1)
        b, d = row_of(g, j), row_of(g, j + 1)
        det = minus(times(a, d), times(b, c))
        scale = 1.0 / (det[0] * det[0] + det[1] * det[1])
        inverse = (det[0] * scale, -det[1] * scale)
        u = minus(times(f, d), times(g, c))
        v = minus(times(g, a), times(f, b))
        u = select(top, (-d[0], -d[1]), select(bottom, c, u))
        v = select(top, b, select(bottom, (-a[0], -a[1]), v))

        def change(x, u, v):
            return plus(times(u, row_of(x, j)), times(v, row_of(x, j + 1)))

        for k in range(j + 2, min(j + 4, STRIP)):
            x = columns[k]
            columns[k] = minus(select(own, none, x), times(change(x, u, v), inverse))
        u, v = times(u, inverse), times(v, inverse)
        for k in range(j + 4, STRIP):
            columns[k] = minus(select(own, none, columns[k]), change(columns[k], u, v))
        rows = minus(select(own, none, rows), change(rows, u, v))
    return rows


def swept(strips, start, sub, lane):
    zero = jnp.zeros_like(strips[0][0])
    count = len(strips)
    for s in range(count):
        first = start + s * STRIP
        columns = [[lane_of(x, first + j) for j in range(STRIP)] for x in strips]
        done = eliminated(strips[s], columns[s], first, sub, lane)
        pivots = [row_of(done, j) for j in range(STRIP)]
        here = (lane >= first) & (lane < first + STRIP)
        for step in range(1, count):
            i = (s + step) % count
            x = select(here, (zero, zero), strips[i])
            for j in range(STRIP):
                x = minus(x, times(columns[i][j], pivots[j]))
            strips[i] = x
        strips[s] = done
    return strips


def thirds(x):
    high = x.astype(jnp.bfloat16)
    rest = x - high.astype(F32)
    middle = rest.astype(jnp.bfloat16)
    return high, middle, (rest - middle.astype(F32)).astype(jnp.bfloat16)


def invert(mats):
    n = mats[0][0].shape[0]
    lane = lax.broadcasted_iota(jnp.int32, (STRIP, n), 1)
    sub = lax.broadcasted_iota(jnp.int32, (STRIP, n), 0)
    wide = lax.broadcasted_iota(jnp.int32, (n, n), 1)
    pair = wide < 2 * PANEL
    even = wide % (2 * PANEL) < PANEL

    def body(step, carry):
        start = pl.multiple_of(step * PANEL, PANEL)
        here = (wide >= start) & (wide < start + PANEL)
        for mat in mats:
            panel = tuple(r[pl.ds(start, PANEL), :] for r in mat)
            strips = [tuple(v[a : a + STRIP, :] for v in panel) for a in range(0, PANEL, STRIP)]
            moved = [
                pltpu.roll(mat[turn % 2][...], n - start + turn * PANEL, 1) for turn in range(4)
            ]
            left = jnp.where(
                pair, jnp.where(even, moved[0], moved[1]), jnp.where(even, moved[2], moved[3])
            )
            high, middle, low = thirds(left)
            left = jnp.concatenate(
                [high, jnp.where(pair, high, middle), jnp.where(pair, middle, low)], axis=1
            )
            strips = swept(strips, start, sub, lane)
            panel = [jnp.concatenate([x[c] for x in strips], axis=0) for c in (0, 1)]
            high, middle, low = thirds(square(panel))
            right = jnp.concatenate([high, middle, low, high, middle, high], axis=0)
            change = halves(jnp.dot(left, right, preferred_element_type=F32))
            for c in (0, 1):
                mat[c][...] = jnp.where(here, 0.0, mat[c][...]) - change[c]
                mat[c][pl.ds(start, PANEL), :] = panel[c]
        return carry

    lax.fori_loop(0, n // PANEL, body, 0)


def packed(x, row, col):
    diagonal = jnp.sum(jnp.where(row == col, x[1], 0.0), axis=0, keepdims=True)
    mean = 0.5 * (jnp.where(row >= col, x[0], x[1]) + jnp.where(row <= col, x[0], x[1]).T)
    return mean, jnp.broadcast_to(diagonal, (STRIP, x[0].shape[1]))


def unpacked(ref, row, col):
    n = ref.shape[1]
    body = ref[0:n, :]
    other = body.T
    diagonal = jnp.broadcast_to(ref[n : n + 1, :], (n, n))
    real = jnp.where(row >= col, body, other)
    imag = jnp.where(row < col, body, jnp.where(row > col, other, diagonal))
    return real, imag


def kernel(
    count, onsite_ref, mixing_ref, strength_ref, hopping_ref, energy_ref, broadening_ref,
    real_ref, imag_ref,
    own_ref, low_ref, high_ref, work, spare, weight_low, weight_high,
    packed_out, packed_low, packed_high, link_low, link_high, from_low, from_high, strength_low,
    pack_up_send, pack_up_recv, pack_down_send, pack_down_recv,
    link_up_send, link_up_recv, link_down_send, link_down_recv, raw_send, raw_recv,
):
    levels = count.bit_length() - 1
    last = levels + 1
    n = mixing_ref.shape[1]
    me = lax.axis_index("slab")
    row = lax.broadcasted_iota(jnp.int32, (n, n), 0)
    col = lax.broadcasted_iota(jnp.int32, (n, n), 1)
    broadening = jnp.where(row == col, broadening_ref[0], 0.0)

    def diagonal(values):
        return jnp.where(row == col, jnp.broadcast_to(values, (n, n)), 0.0)

    def onsite(index):
        mixing = mixing_ref[index]
        hamilton = diagonal(onsite_ref[index : index + 1, :]) + 0.5 * (mixing + mixing.T)
        return jnp.where(row == col, energy_ref[0], 0.0) - hamilton

    def coupling(strengths, hoppings, index):
        return diagonal(strengths[index : index + 1, :]) + hoppings[index]

    def copy(source, target, send, recv, slab):
        return pltpu.make_async_remote_copy(
            src_ref=source, dst_ref=target, send_sem=send, recv_sem=recv,
            device_id={"slab": slab}, device_id_type=MESH,
        )

    def pack_up(slot, slab):
        return copy(packed_out.at[slot], packed_low.at[slot], pack_up_send.at[slot],
                    pack_up_recv.at[slot], slab)

    def pack_down(slot, slab):
        return copy(packed_out.at[slot], packed_high.at[slot], pack_down_send.at[slot],
                    pack_down_recv.at[slot], slab)

    def link_up(slot, slab):
        return copy(link_low.at[slot], from_low.at[slot], link_up_send.at[slot],
                    link_up_recv.at[slot], slab)

    def link_down(slot, slab):
        return copy(link_high.at[slot], from_high.at[slot], link_down_send.at[slot],
                    link_down_recv.at[slot], slab)

    def raw_mixing(slab):
        return copy(hopping_ref, from_low.at[0], raw_send.at[0], raw_recv.at[0], slab)

    def raw_strength(slab):
        return copy(strength_ref, strength_low, raw_send.at[1], raw_recv.at[1], slab)

    def pack(slot, value):
        square_part, tail_part = packed(value, row, col)
        packed_out[slot, 0:n, :] = square_part
        packed_out[slot, n : n + STRIP, :] = tail_part

    def set_work(refs, real):
        refs[0][...] = real
        refs[1][...] = broadening

    def keep(ref, wide_value, sign=None):
        for c, value in enumerate(halves(wide_value)):
            ref[c] = value if sign is None else sign * value

    def add(ref, wide_value):
        for c, value in enumerate(halves(wide_value)):
            ref[c] += value

    def stacked(wide_value):
        return jnp.concatenate(halves(wide_value), axis=0)

    def side_by_side(tall_value):
        return jnp.concatenate([tall_value[:n], tall_value[n:]], axis=1)

    first = (work.at[0], work.at[1])
    second = (spare.at[0], spare.at[1])

    barrier = pltpu.get_barrier_semaphore()
    for level in range(levels):
        stride = 1 << level

        @pl.when(me >= stride)
        def _():
            pl.semaphore_signal(
                barrier, inc=1, device_id={"slab": me - stride}, device_id_type=MESH
            )

        @pl.when(me + stride < count)
        def _():
            pl.semaphore_signal(
                barrier, inc=1, device_id={"slab": me + stride}, device_id_type=MESH
            )

    peers = 0
    for level in range(levels):
        stride = 1 << level
        peers += (me >= stride).astype(jnp.int32) + (me + stride < count).astype(jnp.int32)
    pl.semaphore_wait(barrier, peers)

    @pl.when(me + 1 < count)
    def _():
        raw_mixing(me + 1).start()
        raw_strength(me + 1).start()

    @pl.when(me < 1)
    def _():
        from_low[0] = jnp.zeros((2, n, n), F32)
        strength_low[...] = jnp.zeros((2, n), F32)
        packed_low[0] = jnp.zeros((n + STRIP, n), F32)

    own_ref[...] = onsite(0)
    set_work(first, onsite(1))
    invert((first,))
    pack(0, (first[0][...], first[1][...]))

    @pl.when(me + 1 < count)
    def _():
        pack_up(0, me + 1).start()

    near = coupling(strength_ref, hopping_ref, 0)
    far = jnp.where(me < count - 1, coupling(strength_ref, hopping_ref, 1), 0.0)
    weight = dot(near, beside(unpacked(packed_out.at[0], row, col)))
    keep(weight_high, weight, -1.0)
    keep(high_ref, side_by_side(dot(stacked(weight), near, transpose_b=True)))
    from_high[0, 0] = -far
    from_high[0, 1] = jnp.zeros((n, n), F32)

    @pl.when(me >= 1)
    def _():
        raw_mixing(me).wait_recv()
        raw_strength(me).wait_recv()
        pack_up(0, me).wait_recv()

    near = coupling(strength_low, from_low.at[0], 0)
    far = coupling(strength_low, from_low.at[0], 1)
    weight = dot(far.T, beside(unpacked(packed_low.at[0], row, col)))
    keep(weight_low, weight, -1.0)
    keep(low_ref, side_by_side(dot(stacked(weight), far)))
    from_low[0, 0] = -near.T
    from_low[0, 1] = jnp.zeros((n, n), F32)

    def level_step(level, stride):
        has_low = me >= stride
        has_high = me + stride < count
        inner = jnp.logical_and(has_low, has_high)
        before = level - 1

        first[0][...] = own_ref[...] - low_ref[0] - high_ref[0]
        first[1][...] = broadening - low_ref[1] - high_ref[1]
        invert((first,))
        pack(level, (first[0][...], first[1][...]))

        @pl.when(has_high)
        def _():
            pack_up(level, me + stride).start()

        @pl.when(has_low)
        def _():
            pack_down(level, me - stride).start()

        @pl.when(jnp.logical_and(level > 1, has_low))
        def _():
            link_up(before, me - stride // 2).wait_recv()

        @pl.when(jnp.logical_and(level > 1, has_high))
        def _():
            link_down(before, me + stride // 2).wait_recv()

        @pl.when(jnp.logical_not(has_low))
        def _():
            from_low[before] = jnp.zeros((2, n, n), F32)
            packed_low[level] = jnp.zeros((n + STRIP, n), F32)

        @pl.when(jnp.logical_not(has_high))
        def _():
            from_high[before] = jnp.zeros((2, n, n), F32)
            packed_high[level] = jnp.zeros((n + STRIP, n), F32)

        low = (from_low[before, 0], from_low[before, 1])
        low = dot(beside((weight_low[0], weight_low[1])), square(low))
        keep(link_low.at[level], low, -1.0)
        high = (from_high[before, 0], from_high[before, 1])
        high = dot(beside((weight_high[0], weight_high[1])), square(high))
        keep(link_high.at[level], high, -1.0)

        @pl.when(inner)
        def _():
            link_up(level, me + stride).start()
            link_down(level, me - stride).start()

        @pl.when(level == levels)
        def _():
            second[0][...] = own_ref[...] - jnp.where(has_low, high_ref[0], low_ref[0])
            second[1][...] = broadening - jnp.where(has_low, high_ref[1], low_ref[1])
            invert((second,))

        @pl.when(has_low)
        def _():
            pack_up(level, me - stride).wait_recv()

        @pl.when(has_high)
        def _():
            pack_down(level, me + stride).wait_recv()

        low = (link_low[level, 0], link_low[level, 1])
        high = (link_high[level, 0], link_high[level, 1])
        low_weight = dot(beside(low), square(unpacked(packed_low.at[level], row, col)))
        high_weight = dot(beside(high), square(unpacked(packed_high.at[level], row, col)))
        keep(weight_low, low_weight)
        keep(weight_high, high_weight)
        add(low_ref, dot(low_weight, square_t(low), transpose_b=True))
        add(high_ref, dot(high_weight, square_t(high), transpose_b=True))
        return stride * 2

    lax.fori_loop(1, levels + 1, level_step, 1)

    upper = me >= count // 2
    first[0][...] = own_ref[...] - jnp.where(upper, low_ref[0], high_ref[0])
    first[1][...] = broadening - jnp.where(upper, low_ref[1], high_ref[1])
    invert((first,))
    pack(last, [jnp.where(upper, spare[c], work[c]) for c in (0, 1)])
    left = [jnp.where(upper, work[c], spare[c]) for c in (0, 1)]
    left = [0.5 * (value + value.T) for value in left]
    keep(weight_low, beside(left))

    @pl.when(me >= 1)
    def _():
        pack_down(last, me - 1).start()

    @pl.when(me + 1 >= count)
    def _():
        packed_high[last] = jnp.zeros((n + STRIP, n), F32)

    first[0][...] = own_ref[...] - low_ref[0] - high_ref[0]
    first[1][...] = broadening - low_ref[1] - high_ref[1]
    invert((first,))
    real_ref[0] = first[0][...]
    imag_ref[0] = first[1][...]

    near = coupling(strength_ref, hopping_ref, 0)
    far = jnp.where(me < count - 1, coupling(strength_ref, hopping_ref, 1), 0.0)
    weight = halves(dot(near.T, beside((weight_low[0], weight_low[1]))))
    below = dot(jnp.concatenate([weight[0], weight[1]], axis=0), near)

    @pl.when(me + 1 < count)
    def _():
        pack_down(last, me + 1).wait_recv()

    weight = halves(dot(far, beside(unpacked(packed_high.at[last], row, col))))
    above = dot(jnp.concatenate([weight[0], weight[1]], axis=0), far, transpose_b=True)
    first[0][...] = onsite(1) - below[:n] - above[:n]
    first[1][...] = broadening - below[n:] - above[n:]
    invert((first,))
    real_ref[1] = first[0][...]
    imag_ref[1] = first[1][...]

    @pl.when(me + 1 < count)
    def _():
        raw_mixing(me + 1).wait_send()
        raw_strength(me + 1).wait_send()
        pack_up(0, me + 1).wait_send()

    @pl.when(me >= 1)
    def _():
        pack_down(last, me - 1).wait_send()

    def drain(level, stride):
        has_low = me >= stride
        has_high = me + stride < count

        @pl.when(has_high)
        def _():
            pack_up(level, me + stride).wait_send()

        @pl.when(has_low)
        def _():
            pack_down(level, me - stride).wait_send()

        @pl.when(jnp.logical_and(has_low, has_high))
        def _():
            link_up(level, me + stride).wait_send()
            link_down(level, me - stride).wait_send()

        return stride * 2

    lax.fori_loop(1, levels + 1, drain, 1)


def solution(mesh):
    count = mesh.shape["slab"]
    levels = count.bit_length() - 1

    def shards(onsite_energy, onsite_mixing, hop_strength, hop_mixing, energy, broadening):
        n = onsite_mixing.shape[1]
        whole = pl.BlockSpec(memory_space=pltpu.VMEM)
        scalar = pl.BlockSpec(memory_space=pltpu.SMEM)
        pair = jax.ShapeDtypeStruct((2, n, n), F32)
        pack_shape = pltpu.VMEM((levels + 2, n + STRIP, n), F32)
        link_shape = pltpu.VMEM((levels + 1, 2, n, n), F32)
        sems = pltpu.SemaphoreType.DMA((levels + 2,))
        return pl.pallas_call(
            functools.partial(kernel, count),
            out_shape=(pair, pair),
            in_specs=[whole] * 4 + [scalar] * 2,
            out_specs=(whole, whole),
            scratch_shapes=[
                pltpu.VMEM((n, n), F32),
                pltpu.VMEM((2, n, n), F32),
                pltpu.VMEM((2, n, n), F32),
                pltpu.VMEM((2, n, n), F32),
                pltpu.VMEM((2, n, n), F32),
                pltpu.VMEM((2, n, n), F32),
                pltpu.VMEM((2, n, n), F32),
                pack_shape, pack_shape, pack_shape,
                link_shape, link_shape, link_shape, link_shape,
                pltpu.VMEM((2, n), F32),
            ]
            + [sems] * 8
            + [pltpu.SemaphoreType.DMA((2,))] * 2,
            compiler_params=pltpu.CompilerParams(
                collective_id=0, has_side_effects=True, vmem_limit_bytes=40 * 1024 * 1024
            ),
        )(onsite_energy, onsite_mixing, hop_strength, hop_mixing, energy, broadening)

    return jax.shard_map(
        shards,
        mesh=mesh,
        in_specs=(
            P("slab", None),
            P("slab", None, None),
            P("slab", None),
            P("slab", None, None),
            P("energy"),
            P("energy"),
        ),
        out_specs=(P(("energy", "slab"), None, None), P(("energy", "slab"), None, None)),
        check_vma=False,
    )
```

```python
import functools

import jax
import jax.numpy as jnp
from jax import lax
from jax.experimental import pallas as pl
from jax.experimental.pallas import tpu as pltpu
from jax.sharding import PartitionSpec as P

MESH = pl.DeviceIdType.MESH
F32 = jnp.float32
STRIP = 8
PANEL = 32


def times(a, b):
    return a[0] * b[0] - a[1] * b[1], a[0] * b[1] + a[1] * b[0]


def plus(a, b):
    return a[0] + b[0], a[1] + b[1]


def minus(a, b):
    return a[0] - b[0], a[1] - b[1]


def select(mask, a, b):
    return jnp.where(mask, a[0], b[0]), jnp.where(mask, a[1], b[1])


def row_of(x, j):
    return tuple(jnp.broadcast_to(v[j : j + 1, :], v.shape) for v in x)


def lane_of(x, k):
    lanes = jnp.full(x[0].shape, k, jnp.int32)
    return tuple(jnp.take_along_axis(v, lanes, axis=1) for v in x)


def dot(a, b, transpose_b=False):
    dims = (((1,), (1 if transpose_b else 0,)), ((), ()))
    return lax.dot_general(a, b, dims, precision=lax.Precision.HIGHEST, preferred_element_type=F32)


def beside(x):
    return jnp.concatenate([x[0], x[1]], axis=1)


def square(x):
    top = jnp.concatenate([x[0], x[1]], axis=1)
    return jnp.concatenate([top, jnp.concatenate([-x[1], x[0]], axis=1)], axis=0)


def square_t(x):
    top = jnp.concatenate([x[0], -x[1]], axis=1)
    return jnp.concatenate([top, jnp.concatenate([x[1], x[0]], axis=1)], axis=0)


def halves(x):
    n = x.shape[1] // 2
    return x[:, :n], x[:, n:]


def cdot(a, b):
    return halves(dot(beside(a), square(b)))


def cdot_t(a, b):
    return halves(dot(beside(a), square_t(b), transpose_b=True))


def eliminated(rows, columns, first, sub, lane):
    zero = jnp.zeros_like(rows[0])
    none = (zero, zero)
    eye = jnp.where(lane - first == sub, 1.0, 0.0)
    rows = select((lane >= first) & (lane < first + STRIP), (eye, zero), rows)
    for j in range(0, STRIP, 2):
        top, bottom = sub == j, sub == j + 1
        own = top | bottom
        f, g = columns[j], columns[j + 1]
        a, c = row_of(f, j), row_of(f, j + 1)
        b, d = row_of(g, j), row_of(g, j + 1)
        det = minus(times(a, d), times(b, c))
        scale = 1.0 / (det[0] * det[0] + det[1] * det[1])
        inverse = (det[0] * scale, -det[1] * scale)
        u = minus(times(f, d), times(g, c))
        v = minus(times(g, a), times(f, b))
        u = select(top, (-d[0], -d[1]), select(bottom, c, u))
        v = select(top, b, select(bottom, (-a[0], -a[1]), v))

        def change(x, u, v):
            return plus(times(u, row_of(x, j)), times(v, row_of(x, j + 1)))

        for k in range(j + 2, min(j + 4, STRIP)):
            x = columns[k]
            columns[k] = minus(select(own, none, x), times(change(x, u, v), inverse))
        u, v = times(u, inverse), times(v, inverse)
        for k in range(j + 4, STRIP):
            columns[k] = minus(select(own, none, columns[k]), change(columns[k], u, v))
        rows = minus(select(own, none, rows), change(rows, u, v))
    return rows


def swept(strips, start, sub, lane):
    zero = jnp.zeros_like(strips[0][0])
    count = len(strips)
    for s in range(count):
        first = start + s * STRIP
        columns = [[lane_of(x, first + j) for j in range(STRIP)] for x in strips]
        done = eliminated(strips[s], columns[s], first, sub, lane)
        pivots = [row_of(done, j) for j in range(STRIP)]
        here = (lane >= first) & (lane < first + STRIP)
        for step in range(1, count):
            i = (s + step) % count
            x = select(here, (zero, zero), strips[i])
            for j in range(STRIP):
                x = minus(x, times(columns[i][j], pivots[j]))
            strips[i] = x
        strips[s] = done
    return strips


def thirds(x):
    high = x.astype(jnp.bfloat16)
    rest = x - high.astype(F32)
    middle = rest.astype(jnp.bfloat16)
    return high, middle, (rest - middle.astype(F32)).astype(jnp.bfloat16)


def invert(mats):
    n = mats[0][0].shape[0]
    lane = lax.broadcasted_iota(jnp.int32, (STRIP, n), 1)
    sub = lax.broadcasted_iota(jnp.int32, (STRIP, n), 0)
    wide = lax.broadcasted_iota(jnp.int32, (n, n), 1)
    pair = wide < 2 * PANEL
    even = wide % (2 * PANEL) < PANEL

    def body(step, carry):
        start = pl.multiple_of(step * PANEL, PANEL)
        here = (wide >= start) & (wide < start + PANEL)
        for mat in mats:
            panel = tuple(r[pl.ds(start, PANEL), :] for r in mat)
            strips = [tuple(v[a : a + STRIP, :] for v in panel) for a in range(0, PANEL, STRIP)]
            moved = [
                pltpu.roll(mat[turn % 2][...], n - start + turn * PANEL, 1) for turn in range(4)
            ]
            left = jnp.where(
                pair, jnp.where(even, moved[0], moved[1]), jnp.where(even, moved[2], moved[3])
            )
            high, middle, low = thirds(left)
            left = jnp.concatenate(
                [high, jnp.where(pair, high, middle), jnp.where(pair, middle, low)], axis=1
            )
            strips = swept(strips, start, sub, lane)
            panel = [jnp.concatenate([x[c] for x in strips], axis=0) for c in (0, 1)]
            high, middle, low = thirds(square(panel))
            right = jnp.concatenate([high, middle, low, high, middle, high], axis=0)
            change = halves(jnp.dot(left, right, preferred_element_type=F32))
            for c in (0, 1):
                mat[c][...] = jnp.where(here, 0.0, mat[c][...]) - change[c]
                mat[c][pl.ds(start, PANEL), :] = panel[c]
        return carry

    lax.fori_loop(0, n // PANEL, body, 0)


def packed(x, row, col):
    diagonal = jnp.sum(jnp.where(row == col, x[1], 0.0), axis=0, keepdims=True)
    mean = 0.5 * (jnp.where(row >= col, x[0], x[1]) + jnp.where(row <= col, x[0], x[1]).T)
    return mean, jnp.broadcast_to(diagonal, (STRIP, x[0].shape[1]))


def unpacked(ref, row, col):
    n = ref.shape[1]
    body = ref[0:n, :]
    other = body.T
    diagonal = jnp.broadcast_to(ref[n : n + 1, :], (n, n))
    real = jnp.where(row >= col, body, other)
    imag = jnp.where(row < col, body, jnp.where(row > col, other, diagonal))
    return real, imag


def kernel(
    count, onsite_hbm, mixing_hbm, strength_hbm, hopping_hbm, energy_ref, broadening_ref,
    real_ref, imag_ref,
    onsite_ref, mixing_ref, strength_ref, hopping_ref, input_sem,
    own_ref, low_ref, high_ref, work, spare, weight_low, weight_high,
    packed_out, packed_low, packed_high, link_low, link_high, from_low, from_high,
    pack_up_send, pack_up_recv, pack_down_send, pack_down_recv,
    link_up_send, link_up_recv, link_down_send, link_down_recv,
):
    pieces = [
        pltpu.make_async_copy(source, target, input_sem.at[i])
        for i, (source, target) in enumerate(
            (
                (onsite_hbm, onsite_ref),
                (mixing_hbm, mixing_ref),
                (strength_hbm, strength_ref),
                (hopping_hbm, hopping_ref),
            )
        )
    ]
    for piece in pieces:
        piece.start()

    levels = count.bit_length() - 1
    last = levels + 1
    n = mixing_ref.shape[1]
    me = lax.axis_index("slab")
    row = lax.broadcasted_iota(jnp.int32, (n, n), 0)
    col = lax.broadcasted_iota(jnp.int32, (n, n), 1)
    broadening = jnp.where(row == col, broadening_ref[0], 0.0)

    def diagonal(values):
        return jnp.where(row == col, jnp.broadcast_to(values, (n, n)), 0.0)

    def onsite(index):
        mixing = mixing_ref[index]
        hamilton = diagonal(onsite_ref[index : index + 1, :]) + 0.5 * (mixing + mixing.T)
        return jnp.where(row == col, energy_ref[0], 0.0) - hamilton

    def coupling(strengths, hoppings, index):
        return diagonal(strengths[index : index + 1, :]) + hoppings[index]

    def copy(source, target, send, recv, slab):
        return pltpu.make_async_remote_copy(
            src_ref=source, dst_ref=target, send_sem=send, recv_sem=recv,
            device_id={"slab": slab}, device_id_type=MESH,
        )

    def pack_up(slot, slab):
        return copy(packed_out.at[slot], packed_low.at[slot], pack_up_send.at[slot],
                    pack_up_recv.at[slot], slab)

    def pack_down(slot, slab):
        return copy(packed_out.at[slot], packed_high.at[slot], pack_down_send.at[slot],
                    pack_down_recv.at[slot], slab)

    def link_up(slot, slab):
        return copy(link_low.at[slot], from_low.at[slot], link_up_send.at[slot],
                    link_up_recv.at[slot], slab)

    def link_down(slot, slab):
        return copy(link_high.at[slot], from_high.at[slot], link_down_send.at[slot],
                    link_down_recv.at[slot], slab)

    def pack(slot, value):
        square_part, tail_part = packed(value, row, col)
        packed_out[slot, 0:n, :] = square_part
        packed_out[slot, n : n + STRIP, :] = tail_part

    def keep(ref, wide_value, sign=None):
        for c, value in enumerate(halves(wide_value)):
            ref[c] = value if sign is None else sign * value

    def add(ref, wide_value):
        for c, value in enumerate(halves(wide_value)):
            ref[c] += value

    def stacked(wide_value):
        return jnp.concatenate(halves(wide_value), axis=0)

    def side_by_side(tall_value):
        return jnp.concatenate([tall_value[:n], tall_value[n:]], axis=1)

    first = (work.at[0], work.at[1])
    second = (spare.at[0], spare.at[1])

    barrier = pltpu.get_barrier_semaphore()
    for level in range(levels):
        stride = 1 << level

        @pl.when(me >= stride)
        def _():
            pl.semaphore_signal(
                barrier, inc=1, device_id={"slab": me - stride}, device_id_type=MESH
            )

        @pl.when(me + stride < count)
        def _():
            pl.semaphore_signal(
                barrier, inc=1, device_id={"slab": me + stride}, device_id_type=MESH
            )

    for piece in pieces:
        piece.wait()
    mine = coupling(strength_ref, hopping_ref, 0)
    next_one = jnp.where(me < count - 1, coupling(strength_ref, hopping_ref, 1), 0.0)

    own_ref[...] = onsite(0)
    first[0][...] = onsite(1)
    first[1][...] = broadening
    invert((first,))
    inverse = beside([0.5 * (ref[...] + ref[...].T) for ref in first])
    weight = dot(next_one.T, inverse)
    pack(0, halves(side_by_side(dot(stacked(weight), next_one))))
    peers = 0
    for level in range(levels):
        stride = 1 << level
        peers += (me >= stride).astype(jnp.int32) + (me + stride < count).astype(jnp.int32)
    pl.semaphore_wait(barrier, peers)

    @pl.when(me + 1 < count)
    def _():
        pack_up(0, me + 1).start()

    keep(link_low.at[0], side_by_side(dot(stacked(weight), mine, transpose_b=True)), -1.0)

    @pl.when(me + 1 < count)
    def _():
        link_up(0, me + 1).start()

    @pl.when(me < 1)
    def _():
        from_low[0] = jnp.zeros((2, n, n), F32)
        packed_low[0] = jnp.zeros((n + STRIP, n), F32)

    weight = dot(mine, inverse)
    keep(high_ref, side_by_side(dot(stacked(weight), mine, transpose_b=True)))
    keep(link_high.at[1], side_by_side(dot(stacked(weight), next_one)), -1.0)

    @pl.when(me >= 1)
    def _():
        pack_up(0, me - 1).wait_recv()

    keep(low_ref, beside(unpacked(packed_low.at[0], row, col)))

    def level_step(level, stride):
        has_low = me >= stride
        has_high = me + stride < count
        inner = jnp.logical_and(has_low, has_high)
        before = level - 1

        first[0][...] = own_ref[...] - low_ref[0] - high_ref[0]
        first[1][...] = broadening - low_ref[1] - high_ref[1]
        invert((first,))
        pack(level, (first[0][...], first[1][...]))

        @pl.when(has_high)
        def _():
            pack_up(level, me + stride).start()

        @pl.when(has_low)
        def _():
            pack_down(level, me - stride).start()

        @pl.when(jnp.logical_not(has_low))
        def _():
            packed_low[level] = jnp.zeros((n + STRIP, n), F32)

        @pl.when(jnp.logical_not(has_high))
        def _():
            packed_high[level] = jnp.zeros((n + STRIP, n), F32)

        @pl.when(level == 1)
        def _():
            @pl.when(has_low)
            def _():
                link_up(0, me - 1).wait_recv()

            link_low[1] = from_low[0]

        @pl.when(level > 1)
        def _():
            @pl.when(has_low)
            def _():
                link_up(before, me - stride // 2).wait_recv()

            @pl.when(has_high)
            def _():
                link_down(before, me + stride // 2).wait_recv()

            @pl.when(jnp.logical_not(has_low))
            def _():
                from_low[before] = jnp.zeros((2, n, n), F32)

            @pl.when(jnp.logical_not(has_high))
            def _():
                from_high[before] = jnp.zeros((2, n, n), F32)

            low = (from_low[before, 0], from_low[before, 1])
            low = dot(beside((weight_low[0], weight_low[1])), square(low))
            keep(link_low.at[level], low, -1.0)
            high = (from_high[before, 0], from_high[before, 1])
            high = dot(beside((weight_high[0], weight_high[1])), square(high))
            keep(link_high.at[level], high, -1.0)

        @pl.when(inner)
        def _():
            link_up(level, me + stride).start()
            link_down(level, me - stride).start()

        @pl.when(level == levels)
        def _():
            second[0][...] = own_ref[...] - jnp.where(has_low, high_ref[0], low_ref[0])
            second[1][...] = broadening - jnp.where(has_low, high_ref[1], low_ref[1])
            invert((second,))

        @pl.when(has_low)
        def _():
            pack_up(level, me - stride).wait_recv()

        @pl.when(has_high)
        def _():
            pack_down(level, me + stride).wait_recv()

        low = (link_low[level, 0], link_low[level, 1])
        high = (link_high[level, 0], link_high[level, 1])
        low_weight = dot(beside(low), square(unpacked(packed_low.at[level], row, col)))
        high_weight = dot(beside(high), square(unpacked(packed_high.at[level], row, col)))
        keep(weight_low, low_weight)
        keep(weight_high, high_weight)
        add(low_ref, dot(low_weight, square_t(low), transpose_b=True))
        add(high_ref, dot(high_weight, square_t(high), transpose_b=True))
        return stride * 2

    lax.fori_loop(1, levels + 1, level_step, 1)

    upper = me >= count // 2
    first[0][...] = own_ref[...] - jnp.where(upper, low_ref[0], high_ref[0])
    first[1][...] = broadening - jnp.where(upper, low_ref[1], high_ref[1])
    invert((first,))
    pack(last, [jnp.where(upper, spare[c], work[c]) for c in (0, 1)])
    left = [jnp.where(upper, work[c], spare[c]) for c in (0, 1)]
    left = [0.5 * (value + value.T) for value in left]
    keep(weight_low, beside(left))

    @pl.when(me >= 1)
    def _():
        pack_down(last, me - 1).start()

    @pl.when(me + 1 >= count)
    def _():
        packed_high[last] = jnp.zeros((n + STRIP, n), F32)

    first[0][...] = own_ref[...] - low_ref[0] - high_ref[0]
    first[1][...] = broadening - low_ref[1] - high_ref[1]
    invert((first,))
    real_ref[0] = first[0][...]
    imag_ref[0] = first[1][...]

    weight = halves(dot(mine.T, beside((weight_low[0], weight_low[1]))))
    below = dot(jnp.concatenate([weight[0], weight[1]], axis=0), mine)

    @pl.when(me + 1 < count)
    def _():
        pack_down(last, me + 1).wait_recv()

    weight = halves(dot(next_one, beside(unpacked(packed_high.at[last], row, col))))
    above = dot(jnp.concatenate([weight[0], weight[1]], axis=0), next_one, transpose_b=True)
    first[0][...] = onsite(1) - below[:n] - above[:n]
    first[1][...] = broadening - below[n:] - above[n:]
    invert((first,))
    real_ref[1] = first[0][...]
    imag_ref[1] = first[1][...]

    @pl.when(me + 1 < count)
    def _():
        pack_up(0, me + 1).wait_send()
        link_up(0, me + 1).wait_send()

    @pl.when(me >= 1)
    def _():
        pack_down(last, me - 1).wait_send()

    def drain(level, stride):
        has_low = me >= stride
        has_high = me + stride < count

        @pl.when(has_high)
        def _():
            pack_up(level, me + stride).wait_send()

        @pl.when(has_low)
        def _():
            pack_down(level, me - stride).wait_send()

        @pl.when(jnp.logical_and(has_low, has_high))
        def _():
            link_up(level, me + stride).wait_send()
            link_down(level, me - stride).wait_send()

        return stride * 2

    lax.fori_loop(1, levels + 1, drain, 1)


def solution(mesh):
    count = mesh.shape["slab"]
    levels = count.bit_length() - 1

    def shards(onsite_energy, onsite_mixing, hop_strength, hop_mixing, energy, broadening):
        n = onsite_mixing.shape[1]
        whole = pl.BlockSpec(memory_space=pltpu.VMEM)
        scalar = pl.BlockSpec(memory_space=pltpu.SMEM)
        pair = jax.ShapeDtypeStruct((2, n, n), F32)
        pack_shape = pltpu.VMEM((levels + 2, n + STRIP, n), F32)
        link_shape = pltpu.VMEM((levels + 1, 2, n, n), F32)
        sems = pltpu.SemaphoreType.DMA((levels + 2,))
        return pl.pallas_call(
            functools.partial(kernel, count),
            out_shape=(pair, pair),
            in_specs=[pl.BlockSpec(memory_space=pltpu.HBM)] * 4 + [scalar] * 2,
            out_specs=(whole, whole),
            scratch_shapes=[
                pltpu.VMEM((2, n), F32),
                pltpu.VMEM((2, n, n), F32),
                pltpu.VMEM((2, n), F32),
                pltpu.VMEM((2, n, n), F32),
                pltpu.SemaphoreType.DMA((4,)),
                pltpu.VMEM((n, n), F32),
                pltpu.VMEM((2, n, n), F32),
                pltpu.VMEM((2, n, n), F32),
                pltpu.VMEM((2, n, n), F32),
                pltpu.VMEM((2, n, n), F32),
                pltpu.VMEM((2, n, n), F32),
                pltpu.VMEM((2, n, n), F32),
                pack_shape, pack_shape, pack_shape,
                link_shape, link_shape, link_shape, link_shape,
            ]
            + [sems] * 8,
            compiler_params=pltpu.CompilerParams(
                collective_id=0, has_side_effects=True, vmem_limit_bytes=40 * 1024 * 1024
            ),
        )(onsite_energy, onsite_mixing, hop_strength, hop_mixing, energy, broadening)

    return jax.shard_map(
        shards,
        mesh=mesh,
        in_specs=(
            P("slab", None),
            P("slab", None, None),
            P("slab", None),
            P("slab", None, None),
            P("energy"),
            P("energy"),
        ),
        out_specs=(P(("energy", "slab"), None, None), P(("energy", "slab"), None, None)),
        check_vma=False,
    )
```

```python
import functools

import jax
import jax.numpy as jnp
from jax import lax
from jax.experimental import pallas as pl
from jax.experimental.pallas import tpu as pltpu
from jax.sharding import PartitionSpec as P

MESH = pl.DeviceIdType.MESH
F32 = jnp.float32
STRIP = 8
PANEL = 32


def times(a, b):
    return a[0] * b[0] - a[1] * b[1], a[0] * b[1] + a[1] * b[0]


def plus(a, b):
    return a[0] + b[0], a[1] + b[1]


def minus(a, b):
    return a[0] - b[0], a[1] - b[1]


def select(mask, a, b):
    return jnp.where(mask, a[0], b[0]), jnp.where(mask, a[1], b[1])


def row_of(x, j):
    return tuple(jnp.broadcast_to(v[j : j + 1, :], v.shape) for v in x)


def lane_of(x, k):
    lanes = jnp.full(x[0].shape, k, jnp.int32)
    return tuple(jnp.take_along_axis(v, lanes, axis=1) for v in x)


def dot(a, b, transpose_b=False):
    dims = (((1,), (1 if transpose_b else 0,)), ((), ()))
    return lax.dot_general(a, b, dims, precision=lax.Precision.HIGHEST, preferred_element_type=F32)


def beside(x):
    return jnp.concatenate([x[0], x[1]], axis=1)


def square(x):
    top = jnp.concatenate([x[0], x[1]], axis=1)
    return jnp.concatenate([top, jnp.concatenate([-x[1], x[0]], axis=1)], axis=0)


def square_t(x):
    top = jnp.concatenate([x[0], -x[1]], axis=1)
    return jnp.concatenate([top, jnp.concatenate([x[1], x[0]], axis=1)], axis=0)


def halves(x):
    n = x.shape[1] // 2
    return x[:, :n], x[:, n:]


def cdot(a, b):
    return halves(dot(beside(a), square(b)))


def cdot_t(a, b):
    return halves(dot(beside(a), square_t(b), transpose_b=True))


def eliminated(rows, columns, first, sub, lane):
    zero = jnp.zeros_like(rows[0])
    none = (zero, zero)
    eye = jnp.where(lane - first == sub, 1.0, 0.0)
    rows = select((lane >= first) & (lane < first + STRIP), (eye, zero), rows)
    for j in range(0, STRIP, 2):
        top, bottom = sub == j, sub == j + 1
        own = top | bottom
        f, g = columns[j], columns[j + 1]
        a, c = row_of(f, j), row_of(f, j + 1)
        b, d = row_of(g, j), row_of(g, j + 1)
        det = minus(times(a, d), times(b, c))
        scale = 1.0 / (det[0] * det[0] + det[1] * det[1])
        inverse = (det[0] * scale, -det[1] * scale)
        u = minus(times(f, d), times(g, c))
        v = minus(times(g, a), times(f, b))
        u = select(top, (-d[0], -d[1]), select(bottom, c, u))
        v = select(top, b, select(bottom, (-a[0], -a[1]), v))

        def change(x, u, v):
            return plus(times(u, row_of(x, j)), times(v, row_of(x, j + 1)))

        for k in range(j + 2, min(j + 4, STRIP)):
            x = columns[k]
            columns[k] = minus(select(own, none, x), times(change(x, u, v), inverse))
        u, v = times(u, inverse), times(v, inverse)
        for k in range(j + 4, STRIP):
            columns[k] = minus(select(own, none, columns[k]), change(columns[k], u, v))
        rows = minus(select(own, none, rows), change(rows, u, v))
    return rows


def swept(strips, start, sub, lane):
    zero = jnp.zeros_like(strips[0][0])
    count = len(strips)
    for s in range(count):
        first = start + s * STRIP
        columns = [[lane_of(x, first + j) for j in range(STRIP)] for x in strips]
        done = eliminated(strips[s], columns[s], first, sub, lane)
        pivots = [row_of(done, j) for j in range(STRIP)]
        here = (lane >= first) & (lane < first + STRIP)
        for step in range(1, count):
            i = (s + step) % count
            x = select(here, (zero, zero), strips[i])
            for j in range(STRIP):
                x = minus(x, times(columns[i][j], pivots[j]))
            strips[i] = x
        strips[s] = done
    return strips


def thirds(x):
    high = x.astype(jnp.bfloat16)
    rest = x - high.astype(F32)
    middle = rest.astype(jnp.bfloat16)
    return high, middle, (rest - middle.astype(F32)).astype(jnp.bfloat16)


def invert(mats, low_panel=0, high_panel=None):
    n = mats[0][0].shape[0]
    lane = lax.broadcasted_iota(jnp.int32, (STRIP, n), 1)
    sub = lax.broadcasted_iota(jnp.int32, (STRIP, n), 0)
    wide = lax.broadcasted_iota(jnp.int32, (n, n), 1)
    pair = wide < 2 * PANEL
    even = wide % (2 * PANEL) < PANEL

    def body(step, carry):
        start = pl.multiple_of(step * PANEL, PANEL)
        here = (wide >= start) & (wide < start + PANEL)
        for mat in mats:
            panel = tuple(r[pl.ds(start, PANEL), :] for r in mat)
            strips = [tuple(v[a : a + STRIP, :] for v in panel) for a in range(0, PANEL, STRIP)]
            moved = [
                pltpu.roll(mat[turn % 2][...], n - start + turn * PANEL, 1) for turn in range(4)
            ]
            left = jnp.where(
                pair, jnp.where(even, moved[0], moved[1]), jnp.where(even, moved[2], moved[3])
            )
            high, middle, low = thirds(left)
            left = jnp.concatenate(
                [high, jnp.where(pair, high, middle), jnp.where(pair, middle, low)], axis=1
            )
            strips = swept(strips, start, sub, lane)
            panel = [jnp.concatenate([x[c] for x in strips], axis=0) for c in (0, 1)]
            high, middle, low = thirds(square(panel))
            right = jnp.concatenate([high, middle, low, high, middle, high], axis=0)
            change = halves(jnp.dot(left, right, preferred_element_type=F32))
            for c in (0, 1):
                mat[c][...] = jnp.where(here, 0.0, mat[c][...]) - change[c]
                mat[c][pl.ds(start, PANEL), :] = panel[c]
        return carry

    lax.fori_loop(low_panel, high_panel or n // PANEL, body, 0)


def packed(x, row, col):
    diagonal = jnp.sum(jnp.where(row == col, x[1], 0.0), axis=0, keepdims=True)
    mean = 0.5 * (jnp.where(row >= col, x[0], x[1]) + jnp.where(row <= col, x[0], x[1]).T)
    return mean, jnp.broadcast_to(diagonal, (STRIP, x[0].shape[1]))


def unpacked(ref, row, col):
    n = ref.shape[1]
    body = ref[0:n, :]
    other = body.T
    diagonal = jnp.broadcast_to(ref[n : n + 1, :], (n, n))
    real = jnp.where(row >= col, body, other)
    imag = jnp.where(row < col, body, jnp.where(row > col, other, diagonal))
    return real, imag


def kernel(
    count, onsite_hbm, mixing_hbm, strength_hbm, hopping_hbm, energy_ref, broadening_ref,
    real_ref, imag_ref,
    onsite_ref, mixing_ref, strength_ref, hopping_ref, input_sem,
    own_ref, low_ref, high_ref, work, spare, weight_low, weight_high,
    packed_out, packed_low, packed_high, link_low, link_high, from_low, from_high,
    half_out, half_low, half_high, rest_out, rest_low, rest_high,
    pack_up_send, pack_up_recv, pack_down_send, pack_down_recv,
    link_up_send, link_up_recv, link_down_send, link_down_recv,
    half_up_send, half_up_recv, half_down_send, half_down_recv,
    rest_up_send, rest_up_recv, rest_down_send, rest_down_recv,
):
    pieces = [
        pltpu.make_async_copy(source, target, input_sem.at[i])
        for i, (source, target) in enumerate(
            (
                (onsite_hbm, onsite_ref),
                (mixing_hbm, mixing_ref),
                (strength_hbm, strength_ref),
                (hopping_hbm, hopping_ref),
            )
        )
    ]
    for piece in pieces:
        piece.start()

    levels = count.bit_length() - 1
    last = levels + 1
    n = mixing_ref.shape[1]
    me = lax.axis_index("slab")
    row = lax.broadcasted_iota(jnp.int32, (n, n), 0)
    col = lax.broadcasted_iota(jnp.int32, (n, n), 1)
    broadening = jnp.where(row == col, broadening_ref[0], 0.0)

    def diagonal(values):
        return jnp.where(row == col, jnp.broadcast_to(values, (n, n)), 0.0)

    def onsite(index):
        mixing = mixing_ref[index]
        hamilton = diagonal(onsite_ref[index : index + 1, :]) + 0.5 * (mixing + mixing.T)
        return jnp.where(row == col, energy_ref[0], 0.0) - hamilton

    def coupling(strengths, hoppings, index):
        return diagonal(strengths[index : index + 1, :]) + hoppings[index]

    def copy(source, target, send, recv, slab):
        return pltpu.make_async_remote_copy(
            src_ref=source, dst_ref=target, send_sem=send, recv_sem=recv,
            device_id={"slab": slab}, device_id_type=MESH,
        )

    def pack_up(slot, slab):
        return copy(packed_out.at[slot], packed_low.at[slot], pack_up_send.at[slot],
                    pack_up_recv.at[slot], slab)

    def pack_down(slot, slab):
        return copy(packed_out.at[slot], packed_high.at[slot], pack_down_send.at[slot],
                    pack_down_recv.at[slot], slab)

    def link_up(slot, slab):
        return copy(link_low.at[slot], from_low.at[slot], link_up_send.at[slot],
                    link_up_recv.at[slot], slab)

    def link_down(slot, slab):
        return copy(link_high.at[slot], from_high.at[slot], link_down_send.at[slot],
                    link_down_recv.at[slot], slab)

    def half_up(slot, slab):
        return copy(half_out.at[slot], half_low.at[slot], half_up_send.at[slot],
                    half_up_recv.at[slot], slab)

    def half_down(slot, slab):
        return copy(half_out.at[slot], half_high.at[slot], half_down_send.at[slot],
                    half_down_recv.at[slot], slab)

    def rest_up(slot, slab):
        return copy(rest_out.at[slot], rest_low.at[slot], rest_up_send.at[slot],
                    rest_up_recv.at[slot], slab)

    def rest_down(slot, slab):
        return copy(rest_out.at[slot], rest_high.at[slot], rest_down_send.at[slot],
                    rest_down_recv.at[slot], slab)

    def pack(slot, value):
        square_part, tail_part = packed(value, row, col)
        packed_out[slot, 0:n, :] = square_part
        packed_out[slot, n : n + STRIP, :] = tail_part

    def keep(ref, wide_value, sign=None):
        for c, value in enumerate(halves(wide_value)):
            ref[c] = value if sign is None else sign * value

    def add(ref, wide_value):
        for c, value in enumerate(halves(wide_value)):
            ref[c] += value

    def stacked(wide_value):
        return jnp.concatenate(halves(wide_value), axis=0)

    def side_by_side(tall_value):
        return jnp.concatenate([tall_value[:n], tall_value[n:]], axis=1)

    m = n // 2
    left_lanes = col < m

    def mixed(link, half_ref):
        block = (half_ref[0], half_ref[1])
        lhs = jnp.where(left_lanes, link[0], pltpu.roll(link[1], m, 1))
        product = halves(dot(lhs, square(block)))
        ahead = [
            jnp.where(left_lanes, value, both - value) for value, both in zip(product, link)
        ]
        other = [jnp.where(left_lanes, both, value) for value, both in zip(ahead, link)]
        return ahead, other

    def finished(ahead, rest_ref):
        lhs = jnp.where(left_lanes, pltpu.roll(ahead[0], m, 1), ahead[1])
        rest = rest_ref[...]
        turned = pltpu.roll(rest, m, 1)
        turned = jnp.where(left_lanes[:m], -turned, turned)
        product = dot(lhs, jnp.concatenate([rest, turned], axis=0))
        return (
            jnp.where(left_lanes, ahead[0], pltpu.roll(product, m, 1)),
            jnp.where(left_lanes, ahead[1], product),
        )

    def reduced(link, half_ref):
        turned = [half_ref[c].T[m:, :] for c in (0, 1)]
        change = dot(
            jnp.concatenate(turned, axis=1), square((link[0][:m], link[1][:m]))
        )
        return [
            jnp.concatenate([link[c][:m], link[c][m:] - part], axis=0)
            for c, part in enumerate(halves(change))
        ]

    first = (work.at[0], work.at[1])
    second = (spare.at[0], spare.at[1])

    barrier = pltpu.get_barrier_semaphore()
    for level in range(levels):
        stride = 1 << level

        @pl.when(me >= stride)
        def _():
            pl.semaphore_signal(
                barrier, inc=1, device_id={"slab": me - stride}, device_id_type=MESH
            )

        @pl.when(me + stride < count)
        def _():
            pl.semaphore_signal(
                barrier, inc=1, device_id={"slab": me + stride}, device_id_type=MESH
            )

    for piece in pieces:
        piece.wait()
    mine = coupling(strength_ref, hopping_ref, 0)
    next_one = jnp.where(me < count - 1, coupling(strength_ref, hopping_ref, 1), 0.0)

    own_ref[...] = onsite(0)
    first[0][...] = onsite(1)
    first[1][...] = broadening
    invert((first,))
    inverse = beside([0.5 * (ref[...] + ref[...].T) for ref in first])
    weight = dot(next_one.T, inverse)
    pack(0, halves(side_by_side(dot(stacked(weight), next_one))))
    peers = 0
    for level in range(levels):
        stride = 1 << level
        peers += (me >= stride).astype(jnp.int32) + (me + stride < count).astype(jnp.int32)
    pl.semaphore_wait(barrier, peers)

    @pl.when(me + 1 < count)
    def _():
        pack_up(0, me + 1).start()

    keep(link_low.at[0], side_by_side(dot(stacked(weight), mine, transpose_b=True)), -1.0)

    @pl.when(me + 1 < count)
    def _():
        link_up(0, me + 1).start()

    @pl.when(me < 1)
    def _():
        from_low[0] = jnp.zeros((2, n, n), F32)
        packed_low[0] = jnp.zeros((n + STRIP, n), F32)

    weight = dot(mine, inverse)
    keep(high_ref, side_by_side(dot(stacked(weight), mine, transpose_b=True)))
    keep(link_high.at[1], side_by_side(dot(stacked(weight), next_one)), -1.0)

    @pl.when(me >= 1)
    def _():
        pack_up(0, me - 1).wait_recv()

    keep(low_ref, beside(unpacked(packed_low.at[0], row, col)))

    def level_step(level, stride):
        has_low = me >= stride
        has_high = me + stride < count
        inner = jnp.logical_and(has_low, has_high)
        before = level - 1

        first[0][...] = own_ref[...] - low_ref[0] - high_ref[0]
        first[1][...] = broadening - low_ref[1] - high_ref[1]
        invert((first,), 0, n // PANEL // 2)
        for c in (0, 1):
            turned = first[c][...].T[:m]
            turned = jnp.where(left_lanes[:m], turned, -turned)
            half_out[level, c] = 0.5 * (first[c][0:m, :] + turned)

        @pl.when(has_high)
        def _():
            half_up(level, me + stride).start()

        @pl.when(has_low)
        def _():
            half_down(level, me - stride).start()

        invert((first,), n // PANEL // 2, n // PANEL)
        mean = [0.5 * (ref[m:, :] + ref[...].T[m:]) for ref in first]
        rest_out[level] = jnp.where(left_lanes[:m], pltpu.roll(mean[0], m, 1), mean[1])

        @pl.when(has_high)
        def _():
            rest_up(level, me + stride).start()

        @pl.when(has_low)
        def _():
            rest_down(level, me - stride).start()

        @pl.when(jnp.logical_not(has_low))
        def _():
            half_low[level] = jnp.zeros((2, m, n), F32)
            rest_low[level] = jnp.zeros((m, n), F32)

        @pl.when(jnp.logical_not(has_high))
        def _():
            half_high[level] = jnp.zeros((2, m, n), F32)
            rest_high[level] = jnp.zeros((m, n), F32)

        @pl.when(level == 1)
        def _():
            @pl.when(has_low)
            def _():
                link_up(0, me - 1).wait_recv()

            link_low[1] = from_low[0]

        @pl.when(level > 1)
        def _():
            @pl.when(has_low)
            def _():
                link_up(before, me - stride // 2).wait_recv()

            @pl.when(has_high)
            def _():
                link_down(before, me + stride // 2).wait_recv()

            @pl.when(jnp.logical_not(has_low))
            def _():
                from_low[before] = jnp.zeros((2, n, n), F32)

            @pl.when(jnp.logical_not(has_high))
            def _():
                from_high[before] = jnp.zeros((2, n, n), F32)

            low = (from_low[before, 0], from_low[before, 1])
            low = reduced(low, half_low.at[before])
            low = dot(beside((weight_low[0], weight_low[1])), square(low))
            keep(link_low.at[level], low, -1.0)
            high = (from_high[before, 0], from_high[before, 1])
            high = reduced(high, half_high.at[before])
            high = dot(beside((weight_high[0], weight_high[1])), square(high))
            keep(link_high.at[level], high, -1.0)

        @pl.when(level == levels)
        def _():
            second[0][...] = own_ref[...] - jnp.where(has_low, high_ref[0], low_ref[0])
            second[1][...] = broadening - jnp.where(has_low, high_ref[1], low_ref[1])
            invert((second,))

        @pl.when(has_low)
        def _():
            half_up(level, me - stride).wait_recv()

        @pl.when(has_high)
        def _():
            half_down(level, me + stride).wait_recv()

        low, low_other = mixed((link_low[level, 0], link_low[level, 1]), half_low.at[level])
        high, high_other = mixed((link_high[level, 0], link_high[level, 1]), half_high.at[level])
        low_other = square_t(low_other)
        high_other = square_t(high_other)

        @pl.when(has_low)
        def _():
            rest_up(level, me - stride).wait_recv()

        @pl.when(has_high)
        def _():
            rest_down(level, me + stride).wait_recv()

        @pl.when(inner)
        def _():
            link_up(level, me + stride).start()
            link_down(level, me - stride).start()

        low_weight = beside(finished(low, rest_low.at[level]))
        high_weight = beside(finished(high, rest_high.at[level]))
        add(low_ref, dot(low_weight, low_other, transpose_b=True))
        add(high_ref, dot(high_weight, high_other, transpose_b=True))
        keep(weight_low, low_weight)
        keep(weight_high, high_weight)
        return stride * 2

    lax.fori_loop(1, levels + 1, level_step, 1)

    upper = me >= count // 2
    first[0][...] = own_ref[...] - jnp.where(upper, low_ref[0], high_ref[0])
    first[1][...] = broadening - jnp.where(upper, low_ref[1], high_ref[1])
    invert((first,))
    pack(last, [jnp.where(upper, spare[c], work[c]) for c in (0, 1)])
    left = [jnp.where(upper, work[c], spare[c]) for c in (0, 1)]
    left = [0.5 * (value + value.T) for value in left]
    keep(weight_low, beside(left))

    @pl.when(me >= 1)
    def _():
        pack_down(last, me - 1).start()

    @pl.when(me + 1 >= count)
    def _():
        packed_high[last] = jnp.zeros((n + STRIP, n), F32)

    first[0][...] = own_ref[...] - low_ref[0] - high_ref[0]
    first[1][...] = broadening - low_ref[1] - high_ref[1]
    invert((first,))
    real_ref[0] = first[0][...]
    imag_ref[0] = first[1][...]

    weight = halves(dot(mine.T, beside((weight_low[0], weight_low[1]))))
    below = dot(jnp.concatenate([weight[0], weight[1]], axis=0), mine)

    @pl.when(me + 1 < count)
    def _():
        pack_down(last, me + 1).wait_recv()

    weight = halves(dot(next_one, beside(unpacked(packed_high.at[last], row, col))))
    above = dot(jnp.concatenate([weight[0], weight[1]], axis=0), next_one, transpose_b=True)
    first[0][...] = onsite(1) - below[:n] - above[:n]
    first[1][...] = broadening - below[n:] - above[n:]
    invert((first,))
    real_ref[1] = first[0][...]
    imag_ref[1] = first[1][...]

    @pl.when(me + 1 < count)
    def _():
        pack_up(0, me + 1).wait_send()
        link_up(0, me + 1).wait_send()

    @pl.when(me >= 1)
    def _():
        pack_down(last, me - 1).wait_send()

    def drain(level, stride):
        has_low = me >= stride
        has_high = me + stride < count

        @pl.when(has_high)
        def _():
            half_up(level, me + stride).wait_send()
            rest_up(level, me + stride).wait_send()

        @pl.when(has_low)
        def _():
            half_down(level, me - stride).wait_send()
            rest_down(level, me - stride).wait_send()

        @pl.when(jnp.logical_and(has_low, has_high))
        def _():
            link_up(level, me + stride).wait_send()
            link_down(level, me - stride).wait_send()

        return stride * 2

    lax.fori_loop(1, levels + 1, drain, 1)


def solution(mesh):
    count = mesh.shape["slab"]
    levels = count.bit_length() - 1

    def shards(onsite_energy, onsite_mixing, hop_strength, hop_mixing, energy, broadening):
        n = onsite_mixing.shape[1]
        whole = pl.BlockSpec(memory_space=pltpu.VMEM)
        scalar = pl.BlockSpec(memory_space=pltpu.SMEM)
        pair = jax.ShapeDtypeStruct((2, n, n), F32)
        pack_shape = pltpu.VMEM((levels + 2, n + STRIP, n), F32)
        link_shape = pltpu.VMEM((levels + 1, 2, n, n), F32)
        half_shape = pltpu.VMEM((levels + 1, 2, n // 2, n), F32)
        rest_shape = pltpu.VMEM((levels + 1, n // 2, n), F32)
        sems = pltpu.SemaphoreType.DMA((levels + 2,))
        return pl.pallas_call(
            functools.partial(kernel, count),
            out_shape=(pair, pair),
            in_specs=[pl.BlockSpec(memory_space=pltpu.HBM)] * 4 + [scalar] * 2,
            out_specs=(whole, whole),
            scratch_shapes=[
                pltpu.VMEM((2, n), F32),
                pltpu.VMEM((2, n, n), F32),
                pltpu.VMEM((2, n), F32),
                pltpu.VMEM((2, n, n), F32),
                pltpu.SemaphoreType.DMA((4,)),
                pltpu.VMEM((n, n), F32),
                pltpu.VMEM((2, n, n), F32),
                pltpu.VMEM((2, n, n), F32),
                pltpu.VMEM((2, n, n), F32),
                pltpu.VMEM((2, n, n), F32),
                pltpu.VMEM((2, n, n), F32),
                pltpu.VMEM((2, n, n), F32),
                pack_shape, pack_shape, pack_shape,
                link_shape, link_shape, link_shape, link_shape,
                half_shape, half_shape, half_shape,
                rest_shape, rest_shape, rest_shape,
            ]
            + [sems] * 16,
            compiler_params=pltpu.CompilerParams(
                collective_id=0, has_side_effects=True, vmem_limit_bytes=40 * 1024 * 1024
            ),
        )(onsite_energy, onsite_mixing, hop_strength, hop_mixing, energy, broadening)

    return jax.shard_map(
        shards,
        mesh=mesh,
        in_specs=(
            P("slab", None),
            P("slab", None, None),
            P("slab", None),
            P("slab", None, None),
            P("energy"),
            P("energy"),
        ),
        out_specs=(P(("energy", "slab"), None, None), P(("energy", "slab"), None, None)),
        check_vma=False,
    )
```

```python
import functools

import jax
import jax.numpy as jnp
from jax import lax
from jax.experimental import pallas as pl
from jax.experimental.pallas import tpu as pltpu
from jax.sharding import PartitionSpec as P

MESH = pl.DeviceIdType.MESH
F32 = jnp.float32
STRIP = 8
PANEL = 32


def times(a, b):
    return a[0] * b[0] - a[1] * b[1], a[0] * b[1] + a[1] * b[0]


def plus(a, b):
    return a[0] + b[0], a[1] + b[1]


def minus(a, b):
    return a[0] - b[0], a[1] - b[1]


def select(mask, a, b):
    return jnp.where(mask, a[0], b[0]), jnp.where(mask, a[1], b[1])


def row_of(x, j):
    return tuple(jnp.broadcast_to(v[j : j + 1, :], v.shape) for v in x)


def lane_of(x, k):
    lanes = jnp.full(x[0].shape, k, jnp.int32)
    return tuple(jnp.take_along_axis(v, lanes, axis=1) for v in x)


def dot(a, b, transpose_b=False):
    dims = (((1,), (1 if transpose_b else 0,)), ((), ()))
    return lax.dot_general(a, b, dims, precision=lax.Precision.HIGHEST, preferred_element_type=F32)


def beside(x):
    return jnp.concatenate([x[0], x[1]], axis=1)


def square(x):
    top = jnp.concatenate([x[0], x[1]], axis=1)
    return jnp.concatenate([top, jnp.concatenate([-x[1], x[0]], axis=1)], axis=0)


def square_t(x):
    top = jnp.concatenate([x[0], -x[1]], axis=1)
    return jnp.concatenate([top, jnp.concatenate([x[1], x[0]], axis=1)], axis=0)


def halves(x):
    n = x.shape[1] // 2
    return x[:, :n], x[:, n:]


def cdot(a, b):
    return halves(dot(beside(a), square(b)))


def cdot_t(a, b):
    return halves(dot(beside(a), square_t(b), transpose_b=True))


def eliminated(rows, columns, first, sub, lane):
    zero = jnp.zeros_like(rows[0])
    none = (zero, zero)
    eye = jnp.where(lane - first == sub, 1.0, 0.0)
    rows = select((lane >= first) & (lane < first + STRIP), (eye, zero), rows)
    for j in range(0, STRIP, 2):
        top, bottom = sub == j, sub == j + 1
        own = top | bottom
        f, g = columns[j], columns[j + 1]
        a, c = row_of(f, j), row_of(f, j + 1)
        b, d = row_of(g, j), row_of(g, j + 1)
        det = minus(times(a, d), times(b, c))
        scale = 1.0 / (det[0] * det[0] + det[1] * det[1])
        inverse = (det[0] * scale, -det[1] * scale)
        u = minus(times(f, d), times(g, c))
        v = minus(times(g, a), times(f, b))
        u = select(top, (-d[0], -d[1]), select(bottom, c, u))
        v = select(top, b, select(bottom, (-a[0], -a[1]), v))

        def change(x, u, v):
            return plus(times(u, row_of(x, j)), times(v, row_of(x, j + 1)))

        for k in range(j + 2, min(j + 4, STRIP)):
            x = columns[k]
            columns[k] = minus(select(own, none, x), times(change(x, u, v), inverse))
        u, v = times(u, inverse), times(v, inverse)
        for k in range(j + 4, STRIP):
            columns[k] = minus(select(own, none, columns[k]), change(columns[k], u, v))
        rows = minus(select(own, none, rows), change(rows, u, v))
    return rows


def swept(strips, start, sub, lane):
    zero = jnp.zeros_like(strips[0][0])
    count = len(strips)
    for s in range(count):
        first = start + s * STRIP
        columns = [[lane_of(x, first + j) for j in range(STRIP)] for x in strips]
        done = eliminated(strips[s], columns[s], first, sub, lane)
        pivots = [row_of(done, j) for j in range(STRIP)]
        here = (lane >= first) & (lane < first + STRIP)
        for step in range(1, count):
            i = (s + step) % count
            x = select(here, (zero, zero), strips[i])
            for j in range(STRIP):
                x = minus(x, times(columns[i][j], pivots[j]))
            strips[i] = x
        strips[s] = done
    return strips


def thirds(x):
    high = x.astype(jnp.bfloat16)
    rest = x - high.astype(F32)
    middle = rest.astype(jnp.bfloat16)
    return high, middle, (rest - middle.astype(F32)).astype(jnp.bfloat16)


def invert(mats):
    n = mats[0][0].shape[0]
    lane = lax.broadcasted_iota(jnp.int32, (STRIP, n), 1)
    sub = lax.broadcasted_iota(jnp.int32, (STRIP, n), 0)
    wide = lax.broadcasted_iota(jnp.int32, (n, n), 1)
    pair = wide < 2 * PANEL
    even = wide % (2 * PANEL) < PANEL

    def body(step, carry):
        start = pl.multiple_of(step * PANEL, PANEL)
        here = (wide >= start) & (wide < start + PANEL)
        for mat in mats:
            panel = tuple(r[pl.ds(start, PANEL), :] for r in mat)
            strips = [tuple(v[a : a + STRIP, :] for v in panel) for a in range(0, PANEL, STRIP)]
            moved = [
                pltpu.roll(mat[turn % 2][...], n - start + turn * PANEL, 1) for turn in range(4)
            ]
            left = jnp.where(
                pair, jnp.where(even, moved[0], moved[1]), jnp.where(even, moved[2], moved[3])
            )
            high, middle, low = thirds(left)
            left = jnp.concatenate(
                [high, jnp.where(pair, high, middle), jnp.where(pair, middle, low)], axis=1
            )
            strips = swept(strips, start, sub, lane)
            panel = [jnp.concatenate([x[c] for x in strips], axis=0) for c in (0, 1)]
            high, middle, low = thirds(square(panel))
            right = jnp.concatenate([high, middle, low, high, middle, high], axis=0)
            change = halves(jnp.dot(left, right, preferred_element_type=F32))
            for c in (0, 1):
                mat[c][...] = jnp.where(here, 0.0, mat[c][...]) - change[c]
                mat[c][pl.ds(start, PANEL), :] = panel[c]
        return carry

    lax.fori_loop(0, n // PANEL, body, 0)


def packed(x, row, col):
    diagonal = jnp.sum(jnp.where(row == col, x[1], 0.0), axis=0, keepdims=True)
    mean = 0.5 * (jnp.where(row >= col, x[0], x[1]) + jnp.where(row <= col, x[0], x[1]).T)
    return mean, jnp.broadcast_to(diagonal, (STRIP, x[0].shape[1]))


def unpacked(ref, row, col):
    n = ref.shape[1]
    body = ref[0:n, :]
    other = body.T
    diagonal = jnp.broadcast_to(ref[n : n + 1, :], (n, n))
    real = jnp.where(row >= col, body, other)
    imag = jnp.where(row < col, body, jnp.where(row > col, other, diagonal))
    return real, imag


def kernel(
    count, onsite_hbm, mixing_hbm, strength_hbm, hopping_hbm, energy_ref, broadening_ref,
    real_ref, imag_ref,
    onsite_ref, mixing_ref, strength_ref, hopping_ref, input_sem,
    own_ref, low_ref, high_ref, work, spare, weight_low, weight_high,
    packed_out, packed_low, packed_high, link_low, link_high, from_low, from_high, crossed, cross_sem,
    pack_up_send, pack_up_recv, pack_down_send, pack_down_recv,
    link_up_send, link_up_recv, link_down_send, link_down_recv,
):
    pieces = [
        pltpu.make_async_copy(source, target, input_sem.at[i])
        for i, (source, target) in enumerate(
            (
                (onsite_hbm, onsite_ref),
                (mixing_hbm, mixing_ref),
                (strength_hbm, strength_ref),
                (hopping_hbm, hopping_ref),
            )
        )
    ]
    for piece in pieces:
        piece.start()

    levels = count.bit_length() - 1
    last = levels + 1
    n = mixing_ref.shape[1]
    me = lax.axis_index("slab")
    row = lax.broadcasted_iota(jnp.int32, (n, n), 0)
    col = lax.broadcasted_iota(jnp.int32, (n, n), 1)
    broadening = jnp.where(row == col, broadening_ref[0], 0.0)

    def diagonal(values):
        return jnp.where(row == col, jnp.broadcast_to(values, (n, n)), 0.0)

    def onsite(index):
        mixing = mixing_ref[index]
        hamilton = diagonal(onsite_ref[index : index + 1, :]) + 0.5 * (mixing + mixing.T)
        return jnp.where(row == col, energy_ref[0], 0.0) - hamilton

    def coupling(strengths, hoppings, index):
        return diagonal(strengths[index : index + 1, :]) + hoppings[index]

    def copy(source, target, send, recv, slab):
        return pltpu.make_async_remote_copy(
            src_ref=source, dst_ref=target, send_sem=send, recv_sem=recv,
            device_id={"slab": slab}, device_id_type=MESH,
        )

    def pack_up(slot, slab):
        return copy(packed_out.at[slot], packed_low.at[slot], pack_up_send.at[slot],
                    pack_up_recv.at[slot], slab)

    def pack_down(slot, slab):
        return copy(packed_out.at[slot], packed_high.at[slot], pack_down_send.at[slot],
                    pack_down_recv.at[slot], slab)

    def link_up(slot, slab):
        return copy(link_low.at[slot], from_low.at[slot], link_up_send.at[slot],
                    link_up_recv.at[slot], slab)

    def link_down(slot, slab):
        return copy(link_high.at[slot], from_high.at[slot], link_down_send.at[slot],
                    link_down_recv.at[slot], slab)

    def cross_down(slot, slab):
        return copy(link_low.at[slot], crossed, cross_sem.at[0], cross_sem.at[1], slab)

    def pack(slot, value):
        square_part, tail_part = packed(value, row, col)
        packed_out[slot, 0:n, :] = square_part
        packed_out[slot, n : n + STRIP, :] = tail_part

    def keep(ref, wide_value, sign=None):
        for c, value in enumerate(halves(wide_value)):
            ref[c] = value if sign is None else sign * value

    def add(ref, wide_value):
        for c, value in enumerate(halves(wide_value)):
            ref[c] += value

    def stacked(wide_value):
        return jnp.concatenate(halves(wide_value), axis=0)

    def side_by_side(tall_value):
        return jnp.concatenate([tall_value[:n], tall_value[n:]], axis=1)

    first = (work.at[0], work.at[1])
    second = (spare.at[0], spare.at[1])

    barrier = pltpu.get_barrier_semaphore()
    for level in range(levels):
        stride = 1 << level

        @pl.when(me >= stride)
        def _():
            pl.semaphore_signal(
                barrier, inc=1, device_id={"slab": me - stride}, device_id_type=MESH
            )

        @pl.when(me + stride < count)
        def _():
            pl.semaphore_signal(
                barrier, inc=1, device_id={"slab": me + stride}, device_id_type=MESH
            )

    for piece in pieces:
        piece.wait()
    mine = coupling(strength_ref, hopping_ref, 0)
    next_one = jnp.where(me < count - 1, coupling(strength_ref, hopping_ref, 1), 0.0)

    own_ref[...] = onsite(0)
    first[0][...] = onsite(1)
    first[1][...] = broadening
    invert((first,))
    inverse = beside([0.5 * (ref[...] + ref[...].T) for ref in first])
    weight = dot(next_one.T, inverse)
    pack(0, halves(side_by_side(dot(stacked(weight), next_one))))
    peers = 0
    for level in range(levels):
        stride = 1 << level
        peers += (me >= stride).astype(jnp.int32) + (me + stride < count).astype(jnp.int32)
    pl.semaphore_wait(barrier, peers)

    @pl.when(me + 1 < count)
    def _():
        pack_up(0, me + 1).start()

    keep(link_low.at[0], side_by_side(dot(stacked(weight), mine, transpose_b=True)), -1.0)

    @pl.when(me + 1 < count)
    def _():
        link_up(0, me + 1).start()

    @pl.when(me < 1)
    def _():
        from_low[0] = jnp.zeros((2, n, n), F32)
        packed_low[0] = jnp.zeros((n + STRIP, n), F32)

    weight = dot(mine, inverse)
    keep(high_ref, side_by_side(dot(stacked(weight), mine, transpose_b=True)))
    keep(link_high.at[1], side_by_side(dot(stacked(weight), next_one)), -1.0)

    @pl.when(me >= 1)
    def _():
        pack_up(0, me - 1).wait_recv()

    keep(low_ref, beside(unpacked(packed_low.at[0], row, col)))

    def level_step(level, stride):
        has_low = me >= stride
        has_high = me + stride < count
        inner = jnp.logical_and(has_low, has_high)
        before = level - 1
        crossing = jnp.logical_and(level == levels - 1, level > 1)
        ahead_of_it = jnp.logical_and(level == levels - 2, level >= 1)
        usual = jnp.logical_not(crossing)

        first[0][...] = own_ref[...] - low_ref[0] - high_ref[0]
        first[1][...] = broadening - low_ref[1] - high_ref[1]
        invert((first,))
        pack(level, (first[0][...], first[1][...]))

        @pl.when(has_high)
        def _():
            pack_up(level, me + stride).start()

        @pl.when(has_low)
        def _():
            pack_down(level, me - stride).start()

        @pl.when(jnp.logical_not(has_low))
        def _():
            packed_low[level] = jnp.zeros((n + STRIP, n), F32)

        @pl.when(jnp.logical_not(has_high))
        def _():
            packed_high[level] = jnp.zeros((n + STRIP, n), F32)

        @pl.when(level == 1)
        def _():
            @pl.when(has_low)
            def _():
                link_up(0, me - 1).wait_recv()

            link_low[1] = from_low[0]

        @pl.when(level > 1)
        def _():
            @pl.when(has_low)
            def _():
                link_up(before, me - stride // 2).wait_recv()

            @pl.when(jnp.logical_and(has_high, usual))
            def _():
                link_down(before, me + stride // 2).wait_recv()

            @pl.when(jnp.logical_not(has_low))
            def _():
                from_low[before] = jnp.zeros((2, n, n), F32)

            @pl.when(jnp.logical_not(has_high))
            def _():
                from_high[before] = jnp.zeros((2, n, n), F32)

            low = (from_low[before, 0], from_low[before, 1])
            low = dot(beside((weight_low[0], weight_low[1])), square(low))
            keep(link_low.at[level], low, -1.0)

            @pl.when(usual)
            def _():
                high = (from_high[before, 0], from_high[before, 1])
                high = dot(beside((weight_high[0], weight_high[1])), square(high))
                keep(link_high.at[level], high, -1.0)

            @pl.when(jnp.logical_and(crossing, has_low))
            def _():
                cross_down(level, me - stride).start()

        @pl.when(inner)
        def _():
            link_up(level, me + stride).start()

        @pl.when(jnp.logical_and(inner, jnp.logical_not(jnp.logical_or(crossing, ahead_of_it))))
        def _():
            link_down(level, me - stride).start()

        @pl.when(level == levels)
        def _():
            second[0][...] = own_ref[...] - jnp.where(has_low, high_ref[0], low_ref[0])
            second[1][...] = broadening - jnp.where(has_low, high_ref[1], low_ref[1])
            invert((second,))

        @pl.when(has_low)
        def _():
            pack_up(level, me - stride).wait_recv()

        @pl.when(has_high)
        def _():
            pack_down(level, me + stride).wait_recv()

        def weighed(link, arrived):
            return dot(beside(link), square(unpacked(arrived, row, col)))

        def gained(weight, link):
            return dot(weight, square_t(link), transpose_b=True)

        @pl.when(usual)
        def _():
            low = (link_low[level, 0], link_low[level, 1])
            high = (link_high[level, 0], link_high[level, 1])
            low_weight = weighed(low, packed_low.at[level])
            high_weight = weighed(high, packed_high.at[level])
            keep(weight_low, low_weight)
            keep(weight_high, high_weight)
            add(low_ref, gained(low_weight, low))
            add(high_ref, gained(high_weight, high))

        @pl.when(crossing)
        def _():
            low = (link_low[level, 0], link_low[level, 1])
            low_weight = weighed(low, packed_low.at[level])
            keep(weight_low, low_weight)
            add(low_ref, gained(low_weight, low))

            @pl.when(has_high)
            def _():
                cross_down(level, me + stride).wait_recv()

            @pl.when(jnp.logical_not(has_high))
            def _():
                crossed[...] = jnp.zeros((2, n, n), F32)

            high = (crossed[0].T, crossed[1].T)
            link_high[level, 0] = high[0]
            link_high[level, 1] = high[1]
            high_weight = weighed(high, packed_high.at[level])
            keep(weight_high, high_weight)
            add(high_ref, gained(high_weight, high))

            @pl.when(inner)
            def _():
                link_down(level, me - stride).start()

        return stride * 2

    lax.fori_loop(1, levels + 1, level_step, 1)

    upper = me >= count // 2
    first[0][...] = own_ref[...] - jnp.where(upper, low_ref[0], high_ref[0])
    first[1][...] = broadening - jnp.where(upper, low_ref[1], high_ref[1])
    invert((first,))
    pack(last, [jnp.where(upper, spare[c], work[c]) for c in (0, 1)])
    left = [jnp.where(upper, work[c], spare[c]) for c in (0, 1)]
    left = [0.5 * (value + value.T) for value in left]
    keep(weight_low, beside(left))

    @pl.when(me >= 1)
    def _():
        pack_down(last, me - 1).start()

    @pl.when(me + 1 >= count)
    def _():
        packed_high[last] = jnp.zeros((n + STRIP, n), F32)

    first[0][...] = own_ref[...] - low_ref[0] - high_ref[0]
    first[1][...] = broadening - low_ref[1] - high_ref[1]
    invert((first,))
    real_ref[0] = first[0][...]
    imag_ref[0] = first[1][...]

    weight = halves(dot(mine.T, beside((weight_low[0], weight_low[1]))))
    below = dot(jnp.concatenate([weight[0], weight[1]], axis=0), mine)

    @pl.when(me + 1 < count)
    def _():
        pack_down(last, me + 1).wait_recv()

    weight = halves(dot(next_one, beside(unpacked(packed_high.at[last], row, col))))
    above = dot(jnp.concatenate([weight[0], weight[1]], axis=0), next_one, transpose_b=True)
    first[0][...] = onsite(1) - below[:n] - above[:n]
    first[1][...] = broadening - below[n:] - above[n:]
    invert((first,))
    real_ref[1] = first[0][...]
    imag_ref[1] = first[1][...]

    @pl.when(me + 1 < count)
    def _():
        pack_up(0, me + 1).wait_send()
        link_up(0, me + 1).wait_send()

    @pl.when(me >= 1)
    def _():
        pack_down(last, me - 1).wait_send()

    def drain(level, stride):
        has_low = me >= stride
        has_high = me + stride < count

        @pl.when(has_high)
        def _():
            pack_up(level, me + stride).wait_send()

        @pl.when(has_low)
        def _():
            pack_down(level, me - stride).wait_send()

        crossing = jnp.logical_and(level == levels - 1, level > 1)
        ahead_of_it = jnp.logical_and(level == levels - 2, level >= 1)
        inner = jnp.logical_and(has_low, has_high)

        @pl.when(inner)
        def _():
            link_up(level, me + stride).wait_send()

        @pl.when(jnp.logical_and(inner, jnp.logical_not(ahead_of_it)))
        def _():
            link_down(level, me - stride).wait_send()

        @pl.when(jnp.logical_and(crossing, has_low))
        def _():
            cross_down(level, me - stride).wait_send()

        return stride * 2

    lax.fori_loop(1, levels + 1, drain, 1)


def solution(mesh):
    count = mesh.shape["slab"]
    levels = count.bit_length() - 1

    def shards(onsite_energy, onsite_mixing, hop_strength, hop_mixing, energy, broadening):
        n = onsite_mixing.shape[1]
        whole = pl.BlockSpec(memory_space=pltpu.VMEM)
        scalar = pl.BlockSpec(memory_space=pltpu.SMEM)
        pair = jax.ShapeDtypeStruct((2, n, n), F32)
        pack_shape = pltpu.VMEM((levels + 2, n + STRIP, n), F32)
        link_shape = pltpu.VMEM((levels + 1, 2, n, n), F32)
        sems = pltpu.SemaphoreType.DMA((levels + 2,))
        return pl.pallas_call(
            functools.partial(kernel, count),
            out_shape=(pair, pair),
            in_specs=[pl.BlockSpec(memory_space=pltpu.HBM)] * 4 + [scalar] * 2,
            out_specs=(whole, whole),
            scratch_shapes=[
                pltpu.VMEM((2, n), F32),
                pltpu.VMEM((2, n, n), F32),
                pltpu.VMEM((2, n), F32),
                pltpu.VMEM((2, n, n), F32),
                pltpu.SemaphoreType.DMA((4,)),
                pltpu.VMEM((n, n), F32),
                pltpu.VMEM((2, n, n), F32),
                pltpu.VMEM((2, n, n), F32),
                pltpu.VMEM((2, n, n), F32),
                pltpu.VMEM((2, n, n), F32),
                pltpu.VMEM((2, n, n), F32),
                pltpu.VMEM((2, n, n), F32),
                pack_shape, pack_shape, pack_shape,
                link_shape, link_shape, link_shape, link_shape,
                pltpu.VMEM((2, n, n), F32),
                pltpu.SemaphoreType.DMA((2,)),
            ]
            + [sems] * 8,
            compiler_params=pltpu.CompilerParams(
                collective_id=0, has_side_effects=True, vmem_limit_bytes=40 * 1024 * 1024
            ),
        )(onsite_energy, onsite_mixing, hop_strength, hop_mixing, energy, broadening)

    return jax.shard_map(
        shards,
        mesh=mesh,
        in_specs=(
            P("slab", None),
            P("slab", None, None),
            P("slab", None),
            P("slab", None, None),
            P("energy"),
            P("energy"),
        ),
        out_specs=(P(("energy", "slab"), None, None), P(("energy", "slab"), None, None)),
        check_vma=False,
    )
```

```python
import functools

import jax
import jax.numpy as jnp
from jax import lax
from jax.experimental import pallas as pl
from jax.experimental.pallas import tpu as pltpu
from jax.sharding import PartitionSpec as P

MESH = pl.DeviceIdType.MESH
F32 = jnp.float32
STRIP = 8
PANEL = 32


def times(a, b):
    return a[0] * b[0] - a[1] * b[1], a[0] * b[1] + a[1] * b[0]


def plus(a, b):
    return a[0] + b[0], a[1] + b[1]


def minus(a, b):
    return a[0] - b[0], a[1] - b[1]


def select(mask, a, b):
    return jnp.where(mask, a[0], b[0]), jnp.where(mask, a[1], b[1])


def row_of(x, j):
    return tuple(jnp.broadcast_to(v[j : j + 1, :], v.shape) for v in x)


def lane_of(x, k):
    lanes = jnp.full(x[0].shape, k, jnp.int32)
    return tuple(jnp.take_along_axis(v, lanes, axis=1) for v in x)


def dot(a, b, transpose_b=False):
    dims = (((1,), (1 if transpose_b else 0,)), ((), ()))
    return lax.dot_general(a, b, dims, precision=lax.Precision.HIGHEST, preferred_element_type=F32)


def beside(x):
    return jnp.concatenate([x[0], x[1]], axis=1)


def square(x):
    top = jnp.concatenate([x[0], x[1]], axis=1)
    return jnp.concatenate([top, jnp.concatenate([-x[1], x[0]], axis=1)], axis=0)


def square_t(x):
    top = jnp.concatenate([x[0], -x[1]], axis=1)
    return jnp.concatenate([top, jnp.concatenate([x[1], x[0]], axis=1)], axis=0)


def halves(x):
    n = x.shape[1] // 2
    return x[:, :n], x[:, n:]


def cdot(a, b):
    return halves(dot(beside(a), square(b)))


def cdot_t(a, b):
    return halves(dot(beside(a), square_t(b), transpose_b=True))


def eliminated(rows, columns, first, sub, lane):
    zero = jnp.zeros_like(rows[0])
    none = (zero, zero)
    eye = jnp.where(lane - first == sub, 1.0, 0.0)
    rows = select((lane >= first) & (lane < first + STRIP), (eye, zero), rows)
    for j in range(0, STRIP, 2):
        top, bottom = sub == j, sub == j + 1
        own = top | bottom
        f, g = columns[j], columns[j + 1]
        a, c = row_of(f, j), row_of(f, j + 1)
        b, d = row_of(g, j), row_of(g, j + 1)
        det = minus(times(a, d), times(b, c))
        scale = 1.0 / (det[0] * det[0] + det[1] * det[1])
        inverse = (det[0] * scale, -det[1] * scale)
        u = minus(times(f, d), times(g, c))
        v = minus(times(g, a), times(f, b))
        u = select(top, (-d[0], -d[1]), select(bottom, c, u))
        v = select(top, b, select(bottom, (-a[0], -a[1]), v))

        def change(x, u, v):
            return plus(times(u, row_of(x, j)), times(v, row_of(x, j + 1)))

        for k in range(j + 2, min(j + 4, STRIP)):
            x = columns[k]
            columns[k] = minus(select(own, none, x), times(change(x, u, v), inverse))
        u, v = times(u, inverse), times(v, inverse)
        for k in range(j + 4, STRIP):
            columns[k] = minus(select(own, none, columns[k]), change(columns[k], u, v))
        rows = minus(select(own, none, rows), change(rows, u, v))
    return rows


def swept(strips, start, sub, lane):
    zero = jnp.zeros_like(strips[0][0])
    count = len(strips)
    for s in range(count):
        first = start + s * STRIP
        columns = [[lane_of(x, first + j) for j in range(STRIP)] for x in strips]
        done = eliminated(strips[s], columns[s], first, sub, lane)
        pivots = [row_of(done, j) for j in range(STRIP)]
        here = (lane >= first) & (lane < first + STRIP)
        for step in range(1, count):
            i = (s + step) % count
            x = select(here, (zero, zero), strips[i])
            for j in range(STRIP):
                x = minus(x, times(columns[i][j], pivots[j]))
            strips[i] = x
        strips[s] = done
    return strips


def thirds(x):
    high = x.astype(jnp.bfloat16)
    rest = x - high.astype(F32)
    middle = rest.astype(jnp.bfloat16)
    return high, middle, (rest - middle.astype(F32)).astype(jnp.bfloat16)


def invert(mats):
    n = mats[0][0].shape[0]
    lane = lax.broadcasted_iota(jnp.int32, (STRIP, n), 1)
    sub = lax.broadcasted_iota(jnp.int32, (STRIP, n), 0)
    wide = lax.broadcasted_iota(jnp.int32, (n, n), 1)
    pair = wide < 2 * PANEL
    even = wide % (2 * PANEL) < PANEL

    def body(step, carry):
        start = pl.multiple_of(step * PANEL, PANEL)
        here = (wide >= start) & (wide < start + PANEL)
        for mat in mats:
            panel = tuple(r[pl.ds(start, PANEL), :] for r in mat)
            strips = [tuple(v[a : a + STRIP, :] for v in panel) for a in range(0, PANEL, STRIP)]
            moved = [
                pltpu.roll(mat[turn % 2][...], n - start + turn * PANEL, 1) for turn in range(4)
            ]
            left = jnp.where(
                pair, jnp.where(even, moved[0], moved[1]), jnp.where(even, moved[2], moved[3])
            )
            high, middle, low = thirds(left)
            left = jnp.concatenate(
                [high, jnp.where(pair, high, middle), jnp.where(pair, middle, low)], axis=1
            )
            strips = swept(strips, start, sub, lane)
            panel = [jnp.concatenate([x[c] for x in strips], axis=0) for c in (0, 1)]
            high, middle, low = thirds(square(panel))
            right = jnp.concatenate([high, middle, low, high, middle, high], axis=0)
            change = halves(jnp.dot(left, right, preferred_element_type=F32))
            for c in (0, 1):
                mat[c][...] = jnp.where(here, 0.0, mat[c][...]) - change[c]
                mat[c][pl.ds(start, PANEL), :] = panel[c]
        return carry

    lax.fori_loop(0, n // PANEL, body, 0)


def packed(x, row, col):
    diagonal = jnp.sum(jnp.where(row == col, x[1], 0.0), axis=0, keepdims=True)
    mean = 0.5 * (jnp.where(row >= col, x[0], x[1]) + jnp.where(row <= col, x[0], x[1]).T)
    return mean, jnp.broadcast_to(diagonal, (STRIP, x[0].shape[1]))


def unpacked(ref, row, col):
    n = ref.shape[1]
    body = ref[0:n, :]
    other = body.T
    diagonal = jnp.broadcast_to(ref[n : n + 1, :], (n, n))
    real = jnp.where(row >= col, body, other)
    imag = jnp.where(row < col, body, jnp.where(row > col, other, diagonal))
    return real, imag


def kernel(
    count, onsite_hbm, mixing_hbm, strength_hbm, hopping_hbm, energy_ref, broadening_ref,
    real_ref, imag_ref,
    onsite_ref, mixing_ref, strength_ref, hopping_ref, input_sem,
    own_ref, low_ref, high_ref, work, spare, weight_low, weight_high,
    packed_out, packed_low, packed_high, link_low, link_high, from_low, from_high, crossed, cross_sem,
    pack_up_send, pack_up_recv, pack_down_send, pack_down_recv,
    link_up_send, link_up_recv, link_down_send, link_down_recv,
):
    pieces = [
        pltpu.make_async_copy(source, target, input_sem.at[i])
        for i, (source, target) in enumerate(
            (
                (onsite_hbm, onsite_ref),
                (mixing_hbm, mixing_ref),
                (strength_hbm, strength_ref),
                (hopping_hbm, hopping_ref),
            )
        )
    ]
    for piece in pieces:
        piece.start()

    levels = count.bit_length() - 1
    last = levels + 1
    n = mixing_ref.shape[1]
    me = lax.axis_index("slab")
    row = lax.broadcasted_iota(jnp.int32, (n, n), 0)
    col = lax.broadcasted_iota(jnp.int32, (n, n), 1)
    broadening = jnp.where(row == col, broadening_ref[0], 0.0)

    def diagonal(values):
        return jnp.where(row == col, jnp.broadcast_to(values, (n, n)), 0.0)

    def onsite(index):
        mixing = mixing_ref[index]
        hamilton = diagonal(onsite_ref[index : index + 1, :]) + 0.5 * (mixing + mixing.T)
        return jnp.where(row == col, energy_ref[0], 0.0) - hamilton

    def coupling(strengths, hoppings, index):
        return diagonal(strengths[index : index + 1, :]) + hoppings[index]

    def copy(source, target, send, recv, slab):
        return pltpu.make_async_remote_copy(
            src_ref=source, dst_ref=target, send_sem=send, recv_sem=recv,
            device_id={"slab": slab}, device_id_type=MESH,
        )

    def pack_up(slot, slab):
        return copy(packed_out.at[slot], packed_low.at[slot], pack_up_send.at[slot],
                    pack_up_recv.at[slot], slab)

    def pack_down(slot, slab):
        return copy(packed_out.at[slot], packed_high.at[slot], pack_down_send.at[slot],
                    pack_down_recv.at[slot], slab)

    def link_up(slot, slab):
        return copy(link_low.at[slot], from_low.at[slot], link_up_send.at[slot],
                    link_up_recv.at[slot], slab)

    def link_down(slot, slab):
        return copy(link_high.at[slot], from_high.at[slot], link_down_send.at[slot],
                    link_down_recv.at[slot], slab)

    def cross_down(slot, slab):
        return copy(link_low.at[slot], crossed, cross_sem.at[0], cross_sem.at[1], slab)

    def pack(slot, value):
        square_part, tail_part = packed(value, row, col)
        packed_out[slot, 0:n, :] = square_part
        packed_out[slot, n : n + STRIP, :] = tail_part

    def keep(ref, wide_value, sign=None):
        for c, value in enumerate(halves(wide_value)):
            ref[c] = value if sign is None else sign * value

    def add(ref, wide_value):
        for c, value in enumerate(halves(wide_value)):
            ref[c] += value

    def stacked(wide_value):
        return jnp.concatenate(halves(wide_value), axis=0)

    def side_by_side(tall_value):
        return jnp.concatenate([tall_value[:n], tall_value[n:]], axis=1)

    first = (work.at[0], work.at[1])
    second = (spare.at[0], spare.at[1])

    barrier = pltpu.get_barrier_semaphore()
    for level in range(levels):
        stride = 1 << level

        @pl.when(me >= stride)
        def _():
            pl.semaphore_signal(
                barrier, inc=1, device_id={"slab": me - stride}, device_id_type=MESH
            )

        @pl.when(me + stride < count)
        def _():
            pl.semaphore_signal(
                barrier, inc=1, device_id={"slab": me + stride}, device_id_type=MESH
            )

    for piece in pieces:
        piece.wait()
    mine = coupling(strength_ref, hopping_ref, 0)
    next_one = jnp.where(me < count - 1, coupling(strength_ref, hopping_ref, 1), 0.0)

    first[0][...] = onsite(1)
    first[1][...] = broadening
    invert((first,))
    inverse = beside([0.5 * (ref[...] + ref[...].T) for ref in first])
    weight = dot(next_one.T, inverse)
    pack(0, halves(side_by_side(dot(stacked(weight), next_one))))
    peers = 0
    for level in range(levels):
        stride = 1 << level
        peers += (me >= stride).astype(jnp.int32) + (me + stride < count).astype(jnp.int32)
    pl.semaphore_wait(barrier, peers)

    @pl.when(me + 1 < count)
    def _():
        pack_up(0, me + 1).start()

    keep(link_low.at[0], side_by_side(dot(stacked(weight), mine, transpose_b=True)), -1.0)

    @pl.when(me + 1 < count)
    def _():
        link_up(0, me + 1).start()

    @pl.when(me < 1)
    def _():
        from_low[0] = jnp.zeros((2, n, n), F32)
        packed_low[0] = jnp.zeros((n + STRIP, n), F32)

    own_ref[...] = onsite(0)
    weight = dot(mine, inverse)
    keep(high_ref, side_by_side(dot(stacked(weight), mine, transpose_b=True)))
    keep(link_high.at[1], side_by_side(dot(stacked(weight), next_one)), -1.0)

    @pl.when(me >= 1)
    def _():
        pack_up(0, me - 1).wait_recv()

    keep(low_ref, beside(unpacked(packed_low.at[0], row, col)))

    def level_step(level, stride):
        has_low = me >= stride
        has_high = me + stride < count
        inner = jnp.logical_and(has_low, has_high)
        before = level - 1
        crossing = jnp.logical_and(level == levels - 1, level > 1)
        ahead_of_it = jnp.logical_and(level == levels - 2, level >= 1)
        usual = jnp.logical_not(crossing)

        first[0][...] = own_ref[...] - low_ref[0] - high_ref[0]
        first[1][...] = broadening - low_ref[1] - high_ref[1]
        invert((first,))
        pack(level, (first[0][...], first[1][...]))

        @pl.when(has_high)
        def _():
            pack_up(level, me + stride).start()

        @pl.when(has_low)
        def _():
            pack_down(level, me - stride).start()

        @pl.when(jnp.logical_not(has_low))
        def _():
            packed_low[level] = jnp.zeros((n + STRIP, n), F32)

        @pl.when(jnp.logical_not(has_high))
        def _():
            packed_high[level] = jnp.zeros((n + STRIP, n), F32)

        @pl.when(level == 1)
        def _():
            @pl.when(has_low)
            def _():
                link_up(0, me - 1).wait_recv()

            link_low[1] = from_low[0]

        @pl.when(level > 1)
        def _():
            @pl.when(has_low)
            def _():
                link_up(before, me - stride // 2).wait_recv()

            @pl.when(jnp.logical_and(has_high, usual))
            def _():
                link_down(before, me + stride // 2).wait_recv()

            @pl.when(jnp.logical_not(has_low))
            def _():
                from_low[before] = jnp.zeros((2, n, n), F32)

            @pl.when(jnp.logical_not(has_high))
            def _():
                from_high[before] = jnp.zeros((2, n, n), F32)

            low = (from_low[before, 0], from_low[before, 1])
            low = dot(beside((weight_low[0], weight_low[1])), square(low))
            keep(link_low.at[level], low, -1.0)

            @pl.when(usual)
            def _():
                high = (from_high[before, 0], from_high[before, 1])
                high = dot(beside((weight_high[0], weight_high[1])), square(high))
                keep(link_high.at[level], high, -1.0)

            @pl.when(jnp.logical_and(crossing, has_low))
            def _():
                cross_down(level, me - stride).start()

        @pl.when(inner)
        def _():
            link_up(level, me + stride).start()

        @pl.when(jnp.logical_and(inner, jnp.logical_not(jnp.logical_or(crossing, ahead_of_it))))
        def _():
            link_down(level, me - stride).start()

        @pl.when(level == levels)
        def _():
            second[0][...] = own_ref[...] - jnp.where(has_low, high_ref[0], low_ref[0])
            second[1][...] = broadening - jnp.where(has_low, high_ref[1], low_ref[1])
            invert((second,))

        @pl.when(has_low)
        def _():
            pack_up(level, me - stride).wait_recv()

        @pl.when(has_high)
        def _():
            pack_down(level, me + stride).wait_recv()

        def weighed(link, arrived):
            return dot(beside(link), square(unpacked(arrived, row, col)))

        def gained(weight, link):
            return dot(weight, square_t(link), transpose_b=True)

        @pl.when(usual)
        def _():
            low = (link_low[level, 0], link_low[level, 1])
            high = (link_high[level, 0], link_high[level, 1])
            low_weight = weighed(low, packed_low.at[level])
            high_weight = weighed(high, packed_high.at[level])
            keep(weight_low, low_weight)
            keep(weight_high, high_weight)
            add(low_ref, gained(low_weight, low))
            add(high_ref, gained(high_weight, high))

        @pl.when(crossing)
        def _():
            low = (link_low[level, 0], link_low[level, 1])
            low_weight = weighed(low, packed_low.at[level])
            keep(weight_low, low_weight)
            add(low_ref, gained(low_weight, low))

            @pl.when(has_high)
            def _():
                cross_down(level, me + stride).wait_recv()

            @pl.when(jnp.logical_not(has_high))
            def _():
                crossed[...] = jnp.zeros((2, n, n), F32)

            high = (crossed[0].T, crossed[1].T)
            link_high[level, 0] = high[0]
            link_high[level, 1] = high[1]
            high_weight = weighed(high, packed_high.at[level])
            keep(weight_high, high_weight)
            add(high_ref, gained(high_weight, high))

            @pl.when(inner)
            def _():
                link_down(level, me - stride).start()

        return stride * 2

    lax.fori_loop(1, levels + 1, level_step, 1)

    upper = me >= count // 2
    first[0][...] = own_ref[...] - jnp.where(upper, low_ref[0], high_ref[0])
    first[1][...] = broadening - jnp.where(upper, low_ref[1], high_ref[1])
    invert((first,))
    pack(last, [jnp.where(upper, spare[c], work[c]) for c in (0, 1)])
    @pl.when(me >= 1)
    def _():
        pack_down(last, me - 1).start()

    left = [jnp.where(upper, work[c], spare[c]) for c in (0, 1)]
    left = [0.5 * (value + value.T) for value in left]
    keep(weight_low, beside(left))

    @pl.when(me + 1 >= count)
    def _():
        packed_high[last] = jnp.zeros((n + STRIP, n), F32)

    weight = dot(mine.T, beside((weight_low[0], weight_low[1])))
    keep(weight_high, weight)
    below = dot(stacked(weight), mine)
    second[0][...] = onsite(1) - below[:n]
    second[1][...] = broadening - below[n:]

    @pl.when(me + 1 < count)
    def _():
        pack_down(last, me + 1).wait_recv()

    weight = dot(next_one, beside(unpacked(packed_high.at[last], row, col)))
    above = dot(stacked(weight), next_one, transpose_b=True)
    first[0][...] = second[0][...] - above[:n]
    first[1][...] = second[1][...] - above[n:]
    invert((first,))
    result = (first[0][...], first[1][...])
    real_ref[1] = result[0]
    imag_ref[1] = result[1]
    seen = (weight_high[0], weight_high[1])
    term = cdot((seen[0].T, seen[1].T), result)
    term = cdot(term, seen)
    real_ref[0] = weight_low[0] + term[0]
    imag_ref[0] = weight_low[1] + term[1]

    @pl.when(me + 1 < count)
    def _():
        pack_up(0, me + 1).wait_send()
        link_up(0, me + 1).wait_send()

    @pl.when(me >= 1)
    def _():
        pack_down(last, me - 1).wait_send()

    def drain(level, stride):
        has_low = me >= stride
        has_high = me + stride < count

        @pl.when(has_high)
        def _():
            pack_up(level, me + stride).wait_send()

        @pl.when(has_low)
        def _():
            pack_down(level, me - stride).wait_send()

        crossing = jnp.logical_and(level == levels - 1, level > 1)
        ahead_of_it = jnp.logical_and(level == levels - 2, level >= 1)
        inner = jnp.logical_and(has_low, has_high)

        @pl.when(inner)
        def _():
            link_up(level, me + stride).wait_send()

        @pl.when(jnp.logical_and(inner, jnp.logical_not(ahead_of_it)))
        def _():
            link_down(level, me - stride).wait_send()

        @pl.when(jnp.logical_and(crossing, has_low))
        def _():
            cross_down(level, me - stride).wait_send()

        return stride * 2

    lax.fori_loop(1, levels + 1, drain, 1)


def solution(mesh):
    count = mesh.shape["slab"]
    levels = count.bit_length() - 1

    def shards(onsite_energy, onsite_mixing, hop_strength, hop_mixing, energy, broadening):
        n = onsite_mixing.shape[1]
        whole = pl.BlockSpec(memory_space=pltpu.VMEM)
        scalar = pl.BlockSpec(memory_space=pltpu.SMEM)
        pair = jax.ShapeDtypeStruct((2, n, n), F32)
        pack_shape = pltpu.VMEM((levels + 2, n + STRIP, n), F32)
        link_shape = pltpu.VMEM((levels + 1, 2, n, n), F32)
        sems = pltpu.SemaphoreType.DMA((levels + 2,))
        return pl.pallas_call(
            functools.partial(kernel, count),
            out_shape=(pair, pair),
            in_specs=[pl.BlockSpec(memory_space=pltpu.HBM)] * 4 + [scalar] * 2,
            out_specs=(whole, whole),
            scratch_shapes=[
                pltpu.VMEM((2, n), F32),
                pltpu.VMEM((2, n, n), F32),
                pltpu.VMEM((2, n), F32),
                pltpu.VMEM((2, n, n), F32),
                pltpu.SemaphoreType.DMA((4,)),
                pltpu.VMEM((n, n), F32),
                pltpu.VMEM((2, n, n), F32),
                pltpu.VMEM((2, n, n), F32),
                pltpu.VMEM((2, n, n), F32),
                pltpu.VMEM((2, n, n), F32),
                pltpu.VMEM((2, n, n), F32),
                pltpu.VMEM((2, n, n), F32),
                pack_shape, pack_shape, pack_shape,
                link_shape, link_shape, link_shape, link_shape,
                pltpu.VMEM((2, n, n), F32),
                pltpu.SemaphoreType.DMA((2,)),
            ]
            + [sems] * 8,
            compiler_params=pltpu.CompilerParams(
                collective_id=0, has_side_effects=True, vmem_limit_bytes=40 * 1024 * 1024
            ),
        )(onsite_energy, onsite_mixing, hop_strength, hop_mixing, energy, broadening)

    return jax.shard_map(
        shards,
        mesh=mesh,
        in_specs=(
            P("slab", None),
            P("slab", None, None),
            P("slab", None),
            P("slab", None, None),
            P("energy"),
            P("energy"),
        ),
        out_specs=(P(("energy", "slab"), None, None), P(("energy", "slab"), None, None)),
        check_vma=False,
    )
```

```python
import functools

import jax
import jax.numpy as jnp
from jax import lax
from jax.experimental import pallas as pl
from jax.experimental.pallas import tpu as pltpu
from jax.sharding import PartitionSpec as P

MESH = pl.DeviceIdType.MESH
F32 = jnp.float32
STRIP = 8
PANEL = 32


def times(a, b):
    return a[0] * b[0] - a[1] * b[1], a[0] * b[1] + a[1] * b[0]


def plus(a, b):
    return a[0] + b[0], a[1] + b[1]


def minus(a, b):
    return a[0] - b[0], a[1] - b[1]


def select(mask, a, b):
    return jnp.where(mask, a[0], b[0]), jnp.where(mask, a[1], b[1])


def row_of(x, j):
    return tuple(jnp.broadcast_to(v[j : j + 1, :], v.shape) for v in x)


def lane_of(x, k):
    lanes = jnp.full(x[0].shape, k, jnp.int32)
    return tuple(jnp.take_along_axis(v, lanes, axis=1) for v in x)


def dot(a, b, transpose_b=False):
    dims = (((1,), (1 if transpose_b else 0,)), ((), ()))
    return lax.dot_general(a, b, dims, precision=lax.Precision.HIGHEST, preferred_element_type=F32)


def beside(x):
    return jnp.concatenate([x[0], x[1]], axis=1)


def square(x):
    top = jnp.concatenate([x[0], x[1]], axis=1)
    return jnp.concatenate([top, jnp.concatenate([-x[1], x[0]], axis=1)], axis=0)


def square_t(x):
    top = jnp.concatenate([x[0], -x[1]], axis=1)
    return jnp.concatenate([top, jnp.concatenate([x[1], x[0]], axis=1)], axis=0)


def halves(x):
    n = x.shape[1] // 2
    return x[:, :n], x[:, n:]


def cdot(a, b):
    return halves(dot(beside(a), square(b)))


def cdot_t(a, b):
    return halves(dot(beside(a), square_t(b), transpose_b=True))


def eliminated(rows, columns, first, sub, lane):
    zero = jnp.zeros_like(rows[0])
    none = (zero, zero)
    eye = jnp.where(lane - first == sub, 1.0, 0.0)
    rows = select((lane >= first) & (lane < first + STRIP), (eye, zero), rows)
    for j in range(0, STRIP, 2):
        top, bottom = sub == j, sub == j + 1
        own = top | bottom
        f, g = columns[j], columns[j + 1]
        a, c = row_of(f, j), row_of(f, j + 1)
        b, d = row_of(g, j), row_of(g, j + 1)
        det = minus(times(a, d), times(b, c))
        scale = 1.0 / (det[0] * det[0] + det[1] * det[1])
        inverse = (det[0] * scale, -det[1] * scale)
        u = minus(times(f, d), times(g, c))
        v = minus(times(g, a), times(f, b))
        u = select(top, (-d[0], -d[1]), select(bottom, c, u))
        v = select(top, b, select(bottom, (-a[0], -a[1]), v))

        def change(x, u, v):
            return plus(times(u, row_of(x, j)), times(v, row_of(x, j + 1)))

        for k in range(j + 2, min(j + 4, STRIP)):
            x = columns[k]
            columns[k] = minus(select(own, none, x), times(change(x, u, v), inverse))
        u, v = times(u, inverse), times(v, inverse)
        for k in range(j + 4, STRIP):
            columns[k] = minus(select(own, none, columns[k]), change(columns[k], u, v))
        rows = minus(select(own, none, rows), change(rows, u, v))
    return rows


def swept(strips, start, sub, lane):
    zero = jnp.zeros_like(strips[0][0])
    count = len(strips)
    for s in range(count):
        first = start + s * STRIP
        columns = [[lane_of(x, first + j) for j in range(STRIP)] for x in strips]
        done = eliminated(strips[s], columns[s], first, sub, lane)
        pivots = [row_of(done, j) for j in range(STRIP)]
        here = (lane >= first) & (lane < first + STRIP)
        for step in range(1, count):
            i = (s + step) % count
            x = select(here, (zero, zero), strips[i])
            for j in range(STRIP):
                x = minus(x, times(columns[i][j], pivots[j]))
            strips[i] = x
        strips[s] = done
    return strips


def thirds(x):
    high = x.astype(jnp.bfloat16)
    rest = x - high.astype(F32)
    middle = rest.astype(jnp.bfloat16)
    return high, middle, (rest - middle.astype(F32)).astype(jnp.bfloat16)


def invert(mats):
    n = mats[0][0].shape[0]
    lane = lax.broadcasted_iota(jnp.int32, (STRIP, n), 1)
    sub = lax.broadcasted_iota(jnp.int32, (STRIP, n), 0)
    wide = lax.broadcasted_iota(jnp.int32, (n, n), 1)
    pair = wide < 2 * PANEL
    even = wide % (2 * PANEL) < PANEL

    def body(step, carry):
        start = pl.multiple_of(step * PANEL, PANEL)
        here = (wide >= start) & (wide < start + PANEL)
        for mat in mats:
            panel = tuple(r[pl.ds(start, PANEL), :] for r in mat)
            strips = [tuple(v[a : a + STRIP, :] for v in panel) for a in range(0, PANEL, STRIP)]
            moved = [
                pltpu.roll(mat[turn % 2][...], n - start + turn * PANEL, 1) for turn in range(4)
            ]
            left = jnp.where(
                pair, jnp.where(even, moved[0], moved[1]), jnp.where(even, moved[2], moved[3])
            )
            high, middle, low = thirds(left)
            left = jnp.concatenate(
                [high, jnp.where(pair, high, middle), jnp.where(pair, middle, low)], axis=1
            )
            strips = swept(strips, start, sub, lane)
            panel = [jnp.concatenate([x[c] for x in strips], axis=0) for c in (0, 1)]
            high, middle, low = thirds(square(panel))
            right = jnp.concatenate([high, middle, low, high, middle, high], axis=0)
            change = halves(jnp.dot(left, right, preferred_element_type=F32))
            for c in (0, 1):
                mat[c][...] = jnp.where(here, 0.0, mat[c][...]) - change[c]
                mat[c][pl.ds(start, PANEL), :] = panel[c]
        return carry

    lax.fori_loop(0, n // PANEL, body, 0)


def packed(x, row, col):
    diagonal = jnp.sum(jnp.where(row == col, x[1], 0.0), axis=0, keepdims=True)
    mean = 0.5 * (jnp.where(row >= col, x[0], x[1]) + jnp.where(row <= col, x[0], x[1]).T)
    return mean, jnp.broadcast_to(diagonal, (STRIP, x[0].shape[1]))


def unpacked(ref, row, col):
    n = ref.shape[1]
    body = ref[0:n, :]
    other = body.T
    diagonal = jnp.broadcast_to(ref[n : n + 1, :], (n, n))
    real = jnp.where(row >= col, body, other)
    imag = jnp.where(row < col, body, jnp.where(row > col, other, diagonal))
    return real, imag


def kernel(
    count, onsite_hbm, mixing_hbm, strength_hbm, hopping_hbm, energy_ref, broadening_ref,
    real_ref, imag_ref,
    onsite_ref, mixing_ref, strength_ref, hopping_ref, input_sem,
    own_ref, low_ref, high_ref, work, spare, weight_low, weight_high,
    packed_out, packed_low, packed_high, link_low, link_high, from_low, from_high, crossed, cross_sem,
    pack_up_send, pack_up_recv, pack_down_send, pack_down_recv,
    link_up_send, link_up_recv, link_down_send, link_down_recv,
):
    pieces = [
        pltpu.make_async_copy(source, target, input_sem.at[i])
        for i, (source, target) in enumerate(
            (
                (onsite_hbm, onsite_ref),
                (mixing_hbm, mixing_ref),
                (strength_hbm, strength_ref),
                (hopping_hbm, hopping_ref),
            )
        )
    ]
    for piece in pieces:
        piece.start()

    levels = count.bit_length() - 1
    last = levels + 1
    n = mixing_ref.shape[1]
    me = lax.axis_index("slab")
    row = lax.broadcasted_iota(jnp.int32, (n, n), 0)
    col = lax.broadcasted_iota(jnp.int32, (n, n), 1)
    broadening = jnp.where(row == col, broadening_ref[0], 0.0)

    def diagonal(values):
        return jnp.where(row == col, jnp.broadcast_to(values, (n, n)), 0.0)

    def onsite(index):
        mixing = mixing_ref[index]
        hamilton = diagonal(onsite_ref[index : index + 1, :]) + 0.5 * (mixing + mixing.T)
        return jnp.where(row == col, energy_ref[0], 0.0) - hamilton

    def coupling(strengths, hoppings, index):
        return diagonal(strengths[index : index + 1, :]) + hoppings[index]

    def copy(source, target, send, recv, slab):
        return pltpu.make_async_remote_copy(
            src_ref=source, dst_ref=target, send_sem=send, recv_sem=recv,
            device_id={"slab": slab}, device_id_type=MESH,
        )

    def pack_up(slot, slab):
        return copy(packed_out.at[slot], packed_low.at[slot], pack_up_send.at[slot],
                    pack_up_recv.at[slot], slab)

    def pack_down(slot, slab):
        return copy(packed_out.at[slot], packed_high.at[slot], pack_down_send.at[slot],
                    pack_down_recv.at[slot], slab)

    def link_up(slot, slab):
        return copy(link_low.at[slot], from_low.at[slot], link_up_send.at[slot],
                    link_up_recv.at[slot], slab)

    def link_down(slot, slab):
        return copy(link_high.at[slot], from_high.at[slot], link_down_send.at[slot],
                    link_down_recv.at[slot], slab)

    def cross_down(slot, slab):
        return copy(link_low.at[slot], crossed, cross_sem.at[0], cross_sem.at[1], slab)

    def pack(slot, value):
        square_part, tail_part = packed(value, row, col)
        packed_out[slot, 0:n, :] = square_part
        packed_out[slot, n : n + STRIP, :] = tail_part

    def keep(ref, wide_value, sign=None):
        for c, value in enumerate(halves(wide_value)):
            ref[c] = value if sign is None else sign * value

    def add(ref, wide_value):
        for c, value in enumerate(halves(wide_value)):
            ref[c] += value

    def stacked(wide_value):
        return jnp.concatenate(halves(wide_value), axis=0)

    def side_by_side(tall_value):
        return jnp.concatenate([tall_value[:n], tall_value[n:]], axis=1)

    first = (work.at[0], work.at[1])
    second = (spare.at[0], spare.at[1])

    barrier = pltpu.get_barrier_semaphore()
    for level in range(levels):
        stride = 1 << level

        @pl.when(me >= stride)
        def _():
            pl.semaphore_signal(
                barrier, inc=1, device_id={"slab": me - stride}, device_id_type=MESH
            )

        @pl.when(me + stride < count)
        def _():
            pl.semaphore_signal(
                barrier, inc=1, device_id={"slab": me + stride}, device_id_type=MESH
            )

    for piece in pieces:
        piece.wait()
    mine = coupling(strength_ref, hopping_ref, 0)
    next_one = jnp.where(me < count - 1, coupling(strength_ref, hopping_ref, 1), 0.0)

    first[0][...] = onsite(1)
    first[1][...] = broadening
    invert((first,))
    inverse = beside([0.5 * (ref[...] + ref[...].T) for ref in first])
    weight = dot(next_one.T, inverse)
    pack(0, halves(side_by_side(dot(stacked(weight), next_one))))
    peers = 0
    for level in range(levels):
        stride = 1 << level
        peers += (me >= stride).astype(jnp.int32) + (me + stride < count).astype(jnp.int32)
    pl.semaphore_wait(barrier, peers)

    @pl.when(me + 1 < count)
    def _():
        pack_up(0, me + 1).start()

    keep(link_low.at[0], side_by_side(dot(stacked(weight), mine, transpose_b=True)), -1.0)

    @pl.when(me + 1 < count)
    def _():
        link_up(0, me + 1).start()

    @pl.when(me < 1)
    def _():
        from_low[0] = jnp.zeros((2, n, n), F32)
        packed_low[0] = jnp.zeros((n + STRIP, n), F32)

    own_ref[...] = onsite(0)
    weight = dot(mine, inverse)
    keep(high_ref, side_by_side(dot(stacked(weight), mine, transpose_b=True)))
    keep(link_high.at[1], side_by_side(dot(stacked(weight), next_one)), -1.0)

    @pl.when(me >= 1)
    def _():
        pack_up(0, me - 1).wait_recv()

    keep(low_ref, beside(unpacked(packed_low.at[0], row, col)))

    def level_step(level, stride):
        has_low = me >= stride
        has_high = me + stride < count
        inner = jnp.logical_and(has_low, has_high)
        before = level - 1
        crossing = jnp.logical_and(level == levels - 1, level > 1)
        ahead_of_it = jnp.logical_and(level == levels - 2, level >= 1)
        usual = jnp.logical_not(crossing)

        first[0][...] = own_ref[...] - low_ref[0] - high_ref[0]
        first[1][...] = broadening - low_ref[1] - high_ref[1]
        invert((first,))
        pack(level, (first[0][...], first[1][...]))

        @pl.when(has_high)
        def _():
            pack_up(level, me + stride).start()

        @pl.when(has_low)
        def _():
            pack_down(level, me - stride).start()

        @pl.when(jnp.logical_not(has_low))
        def _():
            packed_low[level] = jnp.zeros((n + STRIP, n), F32)

        @pl.when(jnp.logical_not(has_high))
        def _():
            packed_high[level] = jnp.zeros((n + STRIP, n), F32)

        @pl.when(level == 1)
        def _():
            @pl.when(has_low)
            def _():
                link_up(0, me - 1).wait_recv()

            link_low[1] = from_low[0]

        @pl.when(level > 1)
        def _():
            @pl.when(has_low)
            def _():
                link_up(before, me - stride // 2).wait_recv()

            @pl.when(jnp.logical_and(has_high, usual))
            def _():
                link_down(before, me + stride // 2).wait_recv()

            @pl.when(jnp.logical_not(has_low))
            def _():
                from_low[before] = jnp.zeros((2, n, n), F32)

            @pl.when(jnp.logical_not(has_high))
            def _():
                from_high[before] = jnp.zeros((2, n, n), F32)

            low = (from_low[before, 0], from_low[before, 1])
            low = dot(beside((weight_low[0], weight_low[1])), square(low))
            keep(link_low.at[level], low, -1.0)

            @pl.when(usual)
            def _():
                high = (from_high[before, 0], from_high[before, 1])
                high = dot(beside((weight_high[0], weight_high[1])), square(high))
                keep(link_high.at[level], high, -1.0)

            @pl.when(jnp.logical_and(crossing, has_low))
            def _():
                cross_down(level, me - stride).start()

        @pl.when(inner)
        def _():
            link_up(level, me + stride).start()

        @pl.when(jnp.logical_and(inner, jnp.logical_not(jnp.logical_or(crossing, ahead_of_it))))
        def _():
            link_down(level, me - stride).start()

        @pl.when(level == levels)
        def _():
            second[0][...] = own_ref[...] - jnp.where(has_low, high_ref[0], low_ref[0])
            second[1][...] = broadening - jnp.where(has_low, high_ref[1], low_ref[1])
            invert((second,))

        @pl.when(has_low)
        def _():
            pack_up(level, me - stride).wait_recv()

        @pl.when(has_high)
        def _():
            pack_down(level, me + stride).wait_recv()

        def weighed(link, arrived):
            return dot(beside(link), square(unpacked(arrived, row, col)))

        def gained(weight, link):
            return dot(weight, square_t(link), transpose_b=True)

        @pl.when(jnp.logical_and(level == levels, has_low))
        def _():
            low = (link_low[level, 0], link_low[level, 1])
            add(low_ref, gained(weighed(low, packed_low.at[level]), low))

        @pl.when(jnp.logical_and(level == levels, has_high))
        def _():
            high = (link_high[level, 0], link_high[level, 1])
            add(high_ref, gained(weighed(high, packed_high.at[level]), high))

        @pl.when(jnp.logical_and(usual, level < levels))
        def _():
            low = (link_low[level, 0], link_low[level, 1])
            high = (link_high[level, 0], link_high[level, 1])
            low_weight = weighed(low, packed_low.at[level])
            high_weight = weighed(high, packed_high.at[level])
            keep(weight_low, low_weight)
            keep(weight_high, high_weight)
            add(low_ref, gained(low_weight, low))
            add(high_ref, gained(high_weight, high))

        @pl.when(crossing)
        def _():
            low = (link_low[level, 0], link_low[level, 1])
            low_weight = weighed(low, packed_low.at[level])
            keep(weight_low, low_weight)
            add(low_ref, gained(low_weight, low))

            @pl.when(has_high)
            def _():
                cross_down(level, me + stride).wait_recv()

            @pl.when(jnp.logical_not(has_high))
            def _():
                crossed[...] = jnp.zeros((2, n, n), F32)

            high = (crossed[0].T, crossed[1].T)
            link_high[level, 0] = high[0]
            link_high[level, 1] = high[1]
            high_weight = weighed(high, packed_high.at[level])
            keep(weight_high, high_weight)
            add(high_ref, gained(high_weight, high))

            @pl.when(inner)
            def _():
                link_down(level, me - stride).start()

        return stride * 2

    lax.fori_loop(1, levels + 1, level_step, 1)

    upper = me >= count // 2
    first[0][...] = own_ref[...] - jnp.where(upper, low_ref[0], high_ref[0])
    first[1][...] = broadening - jnp.where(upper, low_ref[1], high_ref[1])
    invert((first,))
    pack(last, [jnp.where(upper, spare[c], work[c]) for c in (0, 1)])
    @pl.when(me >= 1)
    def _():
        pack_down(last, me - 1).start()

    left = [jnp.where(upper, work[c], spare[c]) for c in (0, 1)]
    left = [0.5 * (value + value.T) for value in left]
    keep(weight_low, beside(left))

    @pl.when(me + 1 >= count)
    def _():
        packed_high[last] = jnp.zeros((n + STRIP, n), F32)

    weight = dot(mine.T, beside((weight_low[0], weight_low[1])))
    keep(weight_high, weight)
    below = dot(stacked(weight), mine)
    second[0][...] = onsite(1) - below[:n]
    second[1][...] = broadening - below[n:]

    @pl.when(me + 1 < count)
    def _():
        pack_down(last, me + 1).wait_recv()

    weight = dot(next_one, beside(unpacked(packed_high.at[last], row, col)))
    above = dot(stacked(weight), next_one, transpose_b=True)
    first[0][...] = second[0][...] - above[:n]
    first[1][...] = second[1][...] - above[n:]
    invert((first,))
    result = (first[0][...], first[1][...])
    real_ref[1] = result[0]
    imag_ref[1] = result[1]
    seen = (weight_high[0], weight_high[1])
    term = cdot((seen[0].T, seen[1].T), result)
    term = cdot(term, seen)
    real_ref[0] = weight_low[0] + term[0]
    imag_ref[0] = weight_low[1] + term[1]

    @pl.when(me + 1 < count)
    def _():
        pack_up(0, me + 1).wait_send()
        link_up(0, me + 1).wait_send()

    @pl.when(me >= 1)
    def _():
        pack_down(last, me - 1).wait_send()

    def drain(level, stride):
        has_low = me >= stride
        has_high = me + stride < count

        @pl.when(has_high)
        def _():
            pack_up(level, me + stride).wait_send()

        @pl.when(has_low)
        def _():
            pack_down(level, me - stride).wait_send()

        crossing = jnp.logical_and(level == levels - 1, level > 1)
        ahead_of_it = jnp.logical_and(level == levels - 2, level >= 1)
        inner = jnp.logical_and(has_low, has_high)

        @pl.when(inner)
        def _():
            link_up(level, me + stride).wait_send()

        @pl.when(jnp.logical_and(inner, jnp.logical_not(ahead_of_it)))
        def _():
            link_down(level, me - stride).wait_send()

        @pl.when(jnp.logical_and(crossing, has_low))
        def _():
            cross_down(level, me - stride).wait_send()

        return stride * 2

    lax.fori_loop(1, levels + 1, drain, 1)


def solution(mesh):
    count = mesh.shape["slab"]
    levels = count.bit_length() - 1

    def shards(onsite_energy, onsite_mixing, hop_strength, hop_mixing, energy, broadening):
        n = onsite_mixing.shape[1]
        whole = pl.BlockSpec(memory_space=pltpu.VMEM)
        scalar = pl.BlockSpec(memory_space=pltpu.SMEM)
        pair = jax.ShapeDtypeStruct((2, n, n), F32)
        pack_shape = pltpu.VMEM((levels + 2, n + STRIP, n), F32)
        link_shape = pltpu.VMEM((levels + 1, 2, n, n), F32)
        sems = pltpu.SemaphoreType.DMA((levels + 2,))
        return pl.pallas_call(
            functools.partial(kernel, count),
            out_shape=(pair, pair),
            in_specs=[pl.BlockSpec(memory_space=pltpu.HBM)] * 4 + [scalar] * 2,
            out_specs=(whole, whole),
            scratch_shapes=[
                pltpu.VMEM((2, n), F32),
                pltpu.VMEM((2, n, n), F32),
                pltpu.VMEM((2, n), F32),
                pltpu.VMEM((2, n, n), F32),
                pltpu.SemaphoreType.DMA((4,)),
                pltpu.VMEM((n, n), F32),
                pltpu.VMEM((2, n, n), F32),
                pltpu.VMEM((2, n, n), F32),
                pltpu.VMEM((2, n, n), F32),
                pltpu.VMEM((2, n, n), F32),
                pltpu.VMEM((2, n, n), F32),
                pltpu.VMEM((2, n, n), F32),
                pack_shape, pack_shape, pack_shape,
                link_shape, link_shape, link_shape, link_shape,
                pltpu.VMEM((2, n, n), F32),
                pltpu.SemaphoreType.DMA((2,)),
            ]
            + [sems] * 8,
            compiler_params=pltpu.CompilerParams(
                collective_id=0, has_side_effects=True, vmem_limit_bytes=40 * 1024 * 1024
            ),
        )(onsite_energy, onsite_mixing, hop_strength, hop_mixing, energy, broadening)

    return jax.shard_map(
        shards,
        mesh=mesh,
        in_specs=(
            P("slab", None),
            P("slab", None, None),
            P("slab", None),
            P("slab", None, None),
            P("energy"),
            P("energy"),
        ),
        out_specs=(P(("energy", "slab"), None, None), P(("energy", "slab"), None, None)),
        check_vma=False,
    )
```
